8 devices in a mesh: replica: 1 (over z), model: 8 (over y, x, core).
Axes of the slice: x: 2, y: 2, z: 1, core: 2. Of those that a mesh axis runs over, the one named last changes fastest.
Arguments:
- tokens: bfloat16 [256, 6144], P('replica')
- lengths: int32 [256], P('replica')
- k_cache: bfloat16 [256, 1, 4096, 128], P('replica')
- v_cache: bfloat16 [256, 1, 4096, 128], P('replica')
- norm_gain: bfloat16 [6144], replicated
- w_query: bfloat16 [6144, 6144], P(None, 'model')
- w_key: bfloat16 [6144, 128], replicated
- w_value: bfloat16 [6144, 128], replicated
- w_out: bfloat16 [6144, 6144], P('model')
- w_gate: bfloat16 [6144, 24576], P(None, 'model')
- w_up: bfloat16 [6144, 24576], P(None, 'model')
- w_down: bfloat16 [24576, 6144], P('model')
Outputs:
- output 1: bfloat16 [256, 6144], P('replica')
- output 2: bfloat16 [256, 1, 128], P(('replica', 'model'))
- output 3: bfloat16 [256, 1, 128], P(('replica', 'model'))
All inputs are finite; a program needn't handle non-finite values.
Results may differ from the reference program's by a relative error of at most 0.00437682.
Values are sent between devices in bfloat16 or wider.
A program may use at most 2.75 GiB of HBM per device.

```python
import math
import jax
import jax.numpy as jnp
from jax import lax

MODEL_DIM = 6144
HEADS = 48
KV_HEADS = 1
HEAD_DIM = 128
FFN_DIM = 24576
BATCH_SIZE = 256
CONTEXT = 4096

ROPE_BASE = 10000.0
NORM_EPS = 1e-6
MASK_VALUE = -1e30
KEY_SCALE = math.sqrt(math.log(CONTEXT))
LOG_CONTEXT = int(math.log2(CONTEXT))


def normal_weight(rng_key, fan_in, fan_out, gain):
    return jax.random.normal(rng_key, (fan_in, fan_out), jnp.float32) * (gain / math.sqrt(fan_in))


def setup_inputs(seed: int = 0, part: int = 0) -> dict:
    part_keys = jax.random.split(jax.random.fold_in(jax.random.key(seed), part), 8)
    shared_keys = jax.random.split(jax.random.key(seed + 1), 8)
    query_width = HEADS * HEAD_DIM
    kv_width = KV_HEADS * HEAD_DIM
    tokens = jax.random.normal(part_keys[0], (BATCH_SIZE, MODEL_DIM), jnp.float32)
    spans = jax.random.randint(part_keys[1], (BATCH_SIZE,), 0, CONTEXT - 1)
    shifts = jax.random.randint(part_keys[2], (BATCH_SIZE,), 0, LOG_CONTEXT + 1)
    lengths = 1 + jnp.right_shift(spans, shifts)
    row_ids = jnp.arange(BATCH_SIZE)
    long_row = jax.random.randint(part_keys[3], (), 0, BATCH_SIZE)
    short_row = (long_row + jax.random.randint(part_keys[4], (), 1, BATCH_SIZE)) % BATCH_SIZE
    lengths = jnp.where(row_ids == long_row, CONTEXT - 1, lengths)
    lengths = jnp.where(row_ids == short_row, 1, lengths).astype(jnp.int32)
    cache_shape = (BATCH_SIZE, KV_HEADS, CONTEXT, HEAD_DIM)
    k_cache = jax.random.normal(part_keys[5], cache_shape, jnp.float32) * KEY_SCALE
    v_cache = jax.random.normal(part_keys[6], cache_shape, jnp.float32)
    norm_gain = jax.random.uniform(shared_keys[0], (MODEL_DIM,), jnp.float32, 0.5, 1.5)
    w_query = normal_weight(shared_keys[1], MODEL_DIM, query_width, 1.0)
    w_key = normal_weight(shared_keys[2], MODEL_DIM, kv_width, KEY_SCALE)
    w_value = normal_weight(shared_keys[3], MODEL_DIM, kv_width, 1.0)
    w_out = normal_weight(shared_keys[4], query_width, MODEL_DIM, 1.0)
    w_gate = normal_weight(shared_keys[5], MODEL_DIM, FFN_DIM, 1.0)
    w_up = normal_weight(shared_keys[6], MODEL_DIM, FFN_DIM, 1.0)
    w_down = normal_weight(shared_keys[7], FFN_DIM, MODEL_DIM, 1.0)
    return {
        'tokens': tokens.astype(jnp.bfloat16),
        'lengths': lengths,
        'k_cache': k_cache.astype(jnp.bfloat16),
        'v_cache': v_cache.astype(jnp.bfloat16),
        'norm_gain': norm_gain.astype(jnp.bfloat16),
        'w_query': w_query.astype(jnp.bfloat16),
        'w_key': w_key.astype(jnp.bfloat16),
        'w_value': w_value.astype(jnp.bfloat16),
        'w_out': w_out.astype(jnp.bfloat16),
        'w_gate': w_gate.astype(jnp.bfloat16),
        'w_up': w_up.astype(jnp.bfloat16),
        'w_down': w_down.astype(jnp.bfloat16),
    }


def rms_norm(tokens, norm_gain):
    values = tokens.astype(jnp.float32)
    mean_sq = jnp.mean(values * values, axis=-1, keepdims=True)
    return (values * lax.rsqrt(mean_sq + NORM_EPS) * norm_gain.astype(jnp.float32)).astype(jnp.bfloat16)


def apply_rope(values, positions):
    half_dim = values.shape[-1] // 2
    inv_freq = jnp.exp(jnp.arange(half_dim, dtype=jnp.float32) * (-2.0 * math.log(ROPE_BASE) / values.shape[-1]))
    angles = positions.astype(jnp.float32)[:, None, None] * inv_freq[None, None, :]
    cos_part = jnp.cos(angles)
    sin_part = jnp.sin(angles)
    first_half = values[..., :half_dim]
    second_half = values[..., half_dim:]
    return jnp.concatenate([first_half * cos_part - second_half * sin_part, second_half * cos_part + first_half * sin_part], axis=-1)


def reference(tokens, lengths, k_cache, v_cache, norm_gain, w_query, w_key, w_value, w_out, w_gate, w_up, w_down):
    group_size = HEADS // KV_HEADS
    scale = HEAD_DIM ** -0.5
    normed = rms_norm(tokens, norm_gain)
    queries = apply_rope(jnp.dot(normed, w_query, preferred_element_type=jnp.float32).reshape(BATCH_SIZE, HEADS, HEAD_DIM), lengths).astype(jnp.bfloat16)
    new_keys = apply_rope(jnp.dot(normed, w_key, preferred_element_type=jnp.float32).reshape(BATCH_SIZE, KV_HEADS, HEAD_DIM), lengths).astype(jnp.bfloat16)
    new_values = jnp.dot(normed, w_value, preferred_element_type=jnp.float32).reshape(BATCH_SIZE, KV_HEADS, HEAD_DIM).astype(jnp.bfloat16)
    positions = jnp.arange(CONTEXT)

    def one_sequence(items):
        query_row, key_rows, value_rows, key_new, value_new, length = items
        grouped = query_row.reshape(KV_HEADS, group_size, HEAD_DIM).astype(jnp.float32)
        scores = jnp.einsum('grd,gtd->grt', grouped, key_rows.astype(jnp.float32)) * scale
        scores = jnp.where(positions[None, None, :] < length, scores, MASK_VALUE)
        score_new = jnp.einsum('grd,gd->gr', grouped, key_new.astype(jnp.float32)) * scale
        peak = jnp.maximum(jnp.max(scores, axis=-1), score_new)
        weights = jnp.exp(scores - peak[:, :, None])
        weight_new = jnp.exp(score_new - peak)
        total = jnp.sum(weights, axis=-1) + weight_new
        mixed = jnp.einsum('grt,gtd->grd', weights.astype(jnp.bfloat16).astype(jnp.float32), value_rows.astype(jnp.float32))
        mixed = mixed + weight_new.astype(jnp.bfloat16).astype(jnp.float32)[:, :, None] * value_new.astype(jnp.float32)[:, None, :]
        return (mixed / total[:, :, None]).astype(jnp.bfloat16).reshape(HEADS * HEAD_DIM)

    attended = lax.map(one_sequence, (queries, k_cache, v_cache, new_keys, new_values, lengths))
    gate_act = jnp.dot(normed, w_gate, preferred_element_type=jnp.float32)
    up_act = jnp.dot(normed, w_up, preferred_element_type=jnp.float32)
    hidden = (jax.nn.silu(gate_act) * up_act).astype(jnp.bfloat16)
    summed = tokens.astype(jnp.float32) + jnp.dot(attended, w_out, preferred_element_type=jnp.float32) + jnp.dot(hidden, w_down, preferred_element_type=jnp.float32)
    return summed.astype(jnp.bfloat16), new_keys, new_values
```

```python
import functools
import math
import jax
import jax.numpy as jnp
from jax import lax
from jax.experimental import pallas as pl
from jax.experimental.pallas import tpu as pltpu
from jax.sharding import PartitionSpec as P

ROPE_BASE = 10000.0
NORM_EPS = 1e-6
MASK_VALUE = -1e30
BF16, F32 = jnp.bfloat16, jnp.float32
MESH = pl.DeviceIdType.MESH

PEERS = 8
SLOTS = 3
BLOCK = 512
EARLY = 5
CHUNK = 512
ITEMS = 4
RING = 4
LAGS = (0, 1, 2, 3, 4, 5, 6)


def greet(me):
    barrier = pltpu.get_barrier_semaphore()
    for step in range(1, PEERS):
        peer = lax.rem(me + step, PEERS)
        pl.semaphore_signal(barrier, inc=1, device_id={"model": peer}, device_id_type=MESH)
    return barrier


def gate_up_copies(block, slot, gate_hbm, up_hbm, ring, sems):
    half = BLOCK // 2
    columns = pl.ds(pl.multiple_of(block * half, half), half)
    return (
        pltpu.make_async_copy(gate_hbm.at[:, columns], ring.at[slot, :, pl.ds(0, half)], sems.at[slot, 0]),
        pltpu.make_async_copy(up_hbm.at[:, columns], ring.at[slot, :, pl.ds(half, half)], sems.at[slot, 1]),
    )


def hidden_block(normed, weights):
    half = BLOCK // 2
    both = jnp.dot(normed, weights, preferred_element_type=F32)
    gate, up = both[:, :half], both[:, half:]
    return (gate * lax.logistic(gate) * up).astype(BF16)


def rope(values, cos_part, sin_part):
    return values * cos_part + pltpu.roll(values, 64, 1) * sin_part


def project_kernel(x_hbm, lengths_ref, gain_ref, wq_hbm, wk_hbm, wv_hbm, gate_hbm, up_hbm,
                   q_out, knew_ref, vnew_ref, normed_hbm, hidden_ref,
                   x_ref, normed, ring, q_scr, cos_scr, sin_scr, x_sem, sems, n_sem, send_sem, recv_sem):
    me = lax.axis_index("model")
    batch = x_ref.shape[0]
    rows = batch // PEERS
    barrier = greet(me)
    x_copy = pltpu.make_async_copy(x_hbm, x_ref, x_sem)
    x_copy.start()
    first = (pltpu.make_async_copy(wq_hbm.at[:, pl.ds(0, 512)], ring.at[0], sems.at[0, 0]),)
    second = (
        pltpu.make_async_copy(wq_hbm.at[:, pl.ds(512, 256)], ring.at[1, :, pl.ds(0, 256)], sems.at[1, 0]),
        pltpu.make_async_copy(wk_hbm, ring.at[1, :, pl.ds(256, 128)], sems.at[1, 1]),
        pltpu.make_async_copy(wv_hbm, ring.at[1, :, pl.ds(384, 128)], sems.at[1, 2]),
    )
    gu = lambda block, slot: gate_up_copies(block, slot, gate_hbm, up_hbm, ring, sems)
    for copy in first + second + gu(0, 2):
        copy.start()

    lane = lax.broadcasted_iota(jnp.int32, (batch, 128), 1)
    pair = jnp.where(lane < 64, lane, lane - 64).astype(F32)
    inv_freq = jnp.exp(pair * (-2.0 * math.log(ROPE_BASE) / 128))
    angles = lengths_ref[...].astype(F32) * inv_freq
    cos_scr[...] = jnp.cos(angles)
    sin_scr[...] = jnp.where(lane < 64, -jnp.sin(angles), jnp.sin(angles))

    x_copy.wait()

    def norm_rows(r, _):
        at = pl.ds(pl.multiple_of(r * 16, 16), 16)
        values = x_ref[at, :].astype(F32)
        mean_sq = jnp.mean(values * values, axis=-1, keepdims=True)
        normed[at, :] = (values * lax.rsqrt(mean_sq + NORM_EPS) * gain_ref[...].astype(F32)).astype(BF16)
        return 0

    lax.fori_loop(0, batch // 16, norm_rows, 0)
    n_copy = pltpu.make_async_copy(normed, normed_hbm, n_sem)
    n_copy.start()

    for copy in first:
        copy.wait()
    head4 = jnp.dot(normed[...], ring[0], preferred_element_type=F32)
    for h in range(4):
        q_scr[h] = rope(head4[:, h * 128:(h + 1) * 128], cos_scr[...], sin_scr[...]).astype(BF16)
    if EARLY > 1:
        for copy in gu(1, 0):
            copy.start()
    for copy in second:
        copy.wait()
    tail = jnp.dot(normed[...], ring[1], preferred_element_type=F32)
    for h in range(2):
        q_scr[4 + h] = rope(tail[:, h * 128:(h + 1) * 128], cos_scr[...], sin_scr[...]).astype(BF16)
    k_all = rope(tail[:, 256:384], cos_scr[...], sin_scr[...])
    cos_scr[...] = k_all
    sin_scr[...] = tail[:, 384:512]
    mine = pl.ds(pl.multiple_of(me * rows, rows), rows)
    knew_ref[...] = cos_scr[mine, :].astype(BF16)
    vnew_ref[...] = sin_scr[mine, :].astype(BF16)
    if EARLY > 2:
        for copy in gu(2, 1):
            copy.start()

    pl.semaphore_wait(barrier, PEERS - 1)
    heads = pl.ds(me * 6, 6)
    sends = []
    for step in range(1, PEERS):
        peer = lax.rem(me + step, PEERS)
        sends.append(pltpu.make_async_remote_copy(
            src_ref=q_scr.at[:, pl.ds(pl.multiple_of(peer * rows, rows), rows), :],
            dst_ref=q_out.at[heads],
            send_sem=send_sem.at[step], recv_sem=recv_sem.at[step],
            device_id={"model": peer}, device_id_type=MESH))
        sends[-1].start()
    q_out[heads] = q_scr[:, mine, :]

    half = BLOCK // 2

    def block_step(n, _):
        slot = lax.rem(n + 2, SLOTS)
        for copy in gu(n, slot):
            copy.wait()
        hidden_ref[:, pl.ds(pl.multiple_of(n * half, half), half)] = hidden_block(normed[...], ring[slot])

        @pl.when(n + 3 < EARLY)
        def _():
            for copy in gu(n + 3, slot):
                copy.start()
        return 0

    lax.fori_loop(0, EARLY, block_step, 0)
    for copy in sends:
        copy.wait()
    n_copy.wait()


def attend_kernel(lengths_ref, q_ref, knew_ref, vnew_ref, k_hbm, v_hbm, o_ref,
                  q_scr, o_scr, k_scr, v_scr, k_buf, v_buf, item_row, item_chunk, m_run, l_run, acc_run, k_sem, v_sem):
    me = lax.axis_index("model")
    rows = o_ref.shape[1]
    head_count = o_ref.shape[0]
    base = me * rows
    scale = 128 ** -0.5

    def list_row(b, count):
        chunks = lax.div(lengths_ref[base + b] + (CHUNK - 1), CHUNK)

        def put(c, _):
            item_row[count + c] = b
            item_chunk[count + c] = c
            return 0
        lax.fori_loop(0, chunks, put, 0)
        return count + chunks

    total = lax.fori_loop(0, rows, list_row, jnp.int32(0))
    for extra in range(ITEMS - 1):
        item_row[total + extra] = rows - 1
        item_chunk[total + extra] = 64
    bodies = lax.div(total + (ITEMS - 1), ITEMS)

    def pieces(g, act):
        for j in range(ITEMS):
            n = g * ITEMS + j
            slot = lax.rem(g, RING) * ITEMS + j

            @pl.when(n < total)
            def _():
                b = item_row[n]
                start = item_chunk[n] * CHUNK
                count = jnp.minimum(lax.div(lengths_ref[base + b] - start + 127, 128), CHUNK // 128)

                def piece(p, _):
                    src = pl.ds(pl.multiple_of(start + p * 128, 128), 128)
                    dst = pl.ds(pl.multiple_of(p * 128, 128), 128)
                    act(pltpu.make_async_copy(k_hbm.at[base + b, 0, src, :], k_buf.at[slot, dst, :], k_sem.at[slot]))
                    act(pltpu.make_async_copy(v_hbm.at[base + b, 0, src, :], v_buf.at[slot, dst, :], v_sem.at[slot]))
                    return 0
                lax.fori_loop(0, count, piece, 0)

    k_buf[...] = jnp.zeros_like(k_buf)
    v_buf[...] = jnp.zeros_like(v_buf)
    for g in range(RING - 1):
        pieces(g, lambda copy: copy.start())

    for h in range(head_count):
        q_scr[:, h, :] = q_ref[h].astype(F32)
    k_scr[...] = knew_ref[...].astype(F32)
    v_scr[...] = vnew_ref[...].astype(F32)
    m_run[...] = jnp.zeros_like(m_run)
    l_run[...] = jnp.ones_like(l_run)
    acc_run[...] = jnp.zeros_like(acc_run)

    def body(g, _):
        pieces(g + RING - 1, lambda copy: copy.start())
        pieces(g, lambda copy: copy.wait())
        m, l, acc = m_run[...], l_run[...], acc_run[...]
        scored = []
        for j in range(ITEMS):
            n = g * ITEMS + j
            slot = lax.rem(g, RING) * ITEMS + j
            b, c = item_row[n], item_chunk[n]
            left = lengths_ref[base + b] - c * CHUNK
            q32 = q_scr[b]
            s = lax.dot_general(q32.astype(BF16), k_buf[slot], (((1,), (1,)), ((), ())), preferred_element_type=F32) * scale
            s = jnp.where(lax.broadcasted_iota(jnp.int32, s.shape, 1) < left, s, MASK_VALUE)
            s_new = jnp.sum(q32 * k_scr[pl.ds(b, 1), :], axis=-1, keepdims=True) * scale
            scored.append((s, jnp.max(s, axis=-1, keepdims=True), s_new, b, c, slot))
        for s, s_max, s_new, b, c, slot in scored:
            first = c == 0
            m_prev = jnp.where(first, s_new, m)
            l_prev = jnp.where(first, 1.0, l)
            acc_prev = jnp.where(first, v_scr[pl.ds(b, 1), :], acc)
            m = jnp.maximum(m_prev, s_max)
            e = jnp.exp(s - m)
            shrink = jnp.exp(m_prev - m)
            l = l_prev * shrink + jnp.sum(e, axis=-1, keepdims=True)
            acc = acc_prev * shrink + jnp.dot(e.astype(BF16), v_buf[slot], preferred_element_type=F32)
            o_scr[b] = acc / l
        m_run[...], l_run[...], acc_run[...] = m, l, acc
        return 0

    lax.fori_loop(0, bodies, body, 0)
    for h in range(head_count):
        o_ref[h] = o_scr[:, h, :].astype(BF16)


def combine_kernel(o_ref, x_hbm, normed_hbm, early_hbm, gate_hbm, up_hbm, wo_hbm, wd_hbm, y_ref,
                   normed, act, ring, o_full, x_rows, part, pair_in, in1x, in1y, in2x, in2y,
                   n_sem, e_sem, x_sem, sems, o_send, o_recv, c_send, c_recv):
    me = lax.axis_index("model")
    core = lax.rem(me, 2)
    xi = lax.rem(lax.div(me, 2), 2)
    yi = lax.div(me, 4)
    partner = me + 1 - 2 * core
    x_peer = me + 2 - 4 * xi
    y_peer = me + 4 - 8 * yi
    batch = normed.shape[0]
    rows = batch // PEERS
    late = gate_hbm.shape[1] // (BLOCK // 2) - EARLY
    n_chunks = y_ref.shape[1] // BLOCK
    o_width = wo_hbm.shape[0]
    f_width = wd_hbm.shape[0]
    half = BLOCK // 2
    barrier = greet(me)

    n_copy = pltpu.make_async_copy(normed_hbm, normed, n_sem)
    n_copy.start()
    early_width = EARLY * half
    e_copy = pltpu.make_async_copy(early_hbm, act.at[:, pl.ds(o_width, early_width)], e_sem)

    def gu(n, slot):
        return gate_up_copies(n + EARLY, slot, gate_hbm, up_hbm, ring, sems)

    def down(t, slot):
        columns = pl.ds(pl.multiple_of(t * BLOCK, BLOCK), BLOCK)
        return (
            pltpu.make_async_copy(wo_hbm.at[:, columns], ring.at[slot, pl.ds(0, o_width), :], sems.at[slot, 0]),
            pltpu.make_async_copy(wd_hbm.at[:, columns], ring.at[slot, pl.ds(o_width, f_width), :], sems.at[slot, 1]),
        )

    def fetch(n):
        slot = lax.rem(n, SLOTS)

        @pl.when(n < late)
        def _():
            for copy in gu(n, slot):
                copy.start()

        @pl.when((n >= late) & (n < late + n_chunks))
        def _():
            for copy in down(n - late, slot):
                copy.start()

    for n in range(SLOTS):
        for copy in gu(n, n):
            copy.start()
    e_copy.start()
    row_x = core * 128 + xi * 32 + yi * 16
    row_y = core * 128 + 64 + yi * 32 + xi * 16
    x_copies = []
    for k, row in enumerate((row_x, row_y)):
        x_copies.append(pltpu.make_async_copy(x_hbm.at[pl.ds(pl.multiple_of(row, 16), 16), :], x_rows.at[k], x_sem.at[k]))
        x_copies[-1].start()
    pl.semaphore_wait(barrier, PEERS - 1)
    mine = pl.ds(pl.multiple_of(me * rows, rows), rows)
    sends = []
    for step in range(1, PEERS):
        peer = lax.rem(me + step, PEERS)
        sends.append(pltpu.make_async_remote_copy(
            src_ref=o_ref.at[pl.ds(peer * 6, 6)], dst_ref=o_full.at[:, mine, :],
            send_sem=o_send.at[step], recv_sem=o_recv.at[step],
            device_id={"model": peer}, device_id_type=MESH))
        sends[-1].start()
    o_full[:, mine, :] = o_ref[pl.ds(me * 6, 6)]
    n_copy.wait()

    def block_step(n, _):
        slot = lax.rem(n, SLOTS)
        for copy in gu(n, slot):
            copy.wait()
        at = pl.ds(pl.multiple_of(o_width + early_width + n * half, half), half)
        act[:, at] = hidden_block(normed[...], ring[slot])
        fetch(n + SLOTS)
        return 0

    lax.fori_loop(0, late, block_step, 0)
    e_copy.wait()
    for copy in x_copies:
        copy.wait()
    for copy in sends:
        copy.wait()
    for h in range(6):
        act[:, h * 128:(h + 1) * 128] = o_full[h]

    my_half = pl.multiple_of(core * 128, 128)
    other_half = pl.multiple_of(128 - core * 128, 128)
    keep1x = pl.multiple_of(my_half + xi * 32, 32)
    give1x = pl.multiple_of(my_half + 32 - xi * 32, 32)
    keep1y = pl.multiple_of(my_half + 64 + yi * 32, 32)
    give1y = pl.multiple_of(my_half + 96 - yi * 32, 32)
    keep2x = pl.multiple_of(keep1x + yi * 16, 16)
    give2x = pl.multiple_of(keep1x + 16 - yi * 16, 16)
    keep2y = pl.multiple_of(keep1y + xi * 16, 16)
    give2y = pl.multiple_of(keep1y + 16 - xi * 16, 16)

    def cols(t):
        return pl.ds(pl.multiple_of(t * BLOCK, BLOCK), BLOCK)

    def remote(kind, t, src, dst, peer):
        return pltpu.make_async_remote_copy(
            src_ref=src, dst_ref=dst, send_sem=c_send.at[kind, t], recv_sem=c_recv.at[kind, t],
            device_id={"model": peer}, device_id_type=MESH)

    def pair_sum(t):
        return remote(0, t, part.at[t, pl.ds(other_half, 128), :], pair_in.at[t], partner)

    def scatter1(t):
        return (remote(1, t, part.at[t, pl.ds(give1x, 32), :], in1x.at[t], x_peer),
                remote(2, t, part.at[t, pl.ds(give1y, 32), :], in1y.at[t], y_peer))

    def scatter2(t):
        return (remote(3, t, part.at[t, pl.ds(give2x, 16), :], in2x.at[t], y_peer),
                remote(4, t, part.at[t, pl.ds(give2y, 16), :], in2y.at[t], x_peer))

    def spread(kind, t, row, count, peer):
        at = y_ref.at[pl.ds(row, count), cols(t)]
        return remote(kind, t, at, at, peer)

    def gather1(t):
        return spread(5, t, keep2x, 16, y_peer), spread(6, t, keep2y, 16, x_peer)

    def gather2(t):
        return spread(7, t, keep1x, 32, x_peer), spread(8, t, keep1y, 32, y_peer)

    def pair_copy(t):
        return (spread(9, t, my_half, 128, partner),)

    def start(copies):
        for copy in copies:
            copy.start()

    def arrive(copies):
        for copy in copies:
            copy.wait_recv()

    def stage_compute(t):
        slot = lax.rem(t + late, SLOTS)
        for copy in down(t, slot):
            copy.wait()
        part[t] = jnp.dot(act[...], ring[slot, pl.ds(0, o_width + f_width), :], preferred_element_type=F32)
        pair_sum(t).start()
        fetch(t + late + SLOTS)

    def stage_scatter1(t):
        pair_sum(t).wait_recv()
        part[t, pl.ds(my_half, 128), :] = part[t, pl.ds(my_half, 128), :] + pair_in[t]
        start(scatter1(t))

    def stage_scatter2(t):
        arrive(scatter1(t))
        part[t, pl.ds(keep1x, 32), :] = part[t, pl.ds(keep1x, 32), :] + in1x[t]
        part[t, pl.ds(keep1y, 32), :] = part[t, pl.ds(keep1y, 32), :] + in1y[t]
        start(scatter2(t))

    def stage_gather1(t):
        arrive(scatter2(t))
        for k, (keep, inbox) in enumerate(((keep2x, in2x), (keep2y, in2y))):
            total = part[t, pl.ds(keep, 16), :] + inbox[t]
            y_ref[pl.ds(keep, 16), cols(t)] = (x_rows[k, :, cols(t)].astype(F32) + total).astype(BF16)
        start(gather1(t))

    def stage_gather2(t):
        arrive(gather1(t))
        start(gather2(t))

    def stage_pair(t):
        arrive(gather2(t))
        start(pair_copy(t))

    def stage_end(t):
        arrive(pair_copy(t))

    stages = (stage_compute, stage_scatter1, stage_scatter2, stage_gather1, stage_gather2, stage_pair, stage_end)

    def iteration(i, _):
        for lag, stage in zip(LAGS, stages):
            t = i - lag

            @pl.when((t >= 0) & (t < n_chunks))
            def _(stage=stage, t=t):
                stage(t)
        return 0

    lax.fori_loop(0, n_chunks + LAGS[-1], iteration, 0)

    def drain(t, _):
        for copy in (pair_sum(t),) + scatter1(t) + scatter2(t) + gather1(t) + gather2(t) + pair_copy(t):
            copy.wait_send()
        return 0

    lax.fori_loop(0, n_chunks, drain, 0)


ANY = pl.BlockSpec(memory_space=pl.ANY)
VM = pl.BlockSpec(memory_space=pltpu.VMEM)
SM = pl.BlockSpec(memory_space=pltpu.SMEM)
LIMIT = 62 << 20


def solution(mesh):
    def local_step(tokens, lengths, k_cache, v_cache, norm_gain, w_query, w_key, w_value, w_out, w_gate, w_up, w_down):
        batch, width = tokens.shape
        rows = batch // PEERS
        heads = width // 128
        n_chunks = width // BLOCK
        dma = pltpu.SemaphoreType.DMA

        q_all, key_new, value_new, normed, early = pl.pallas_call(
            project_kernel,
            name="project",
            out_shape=(
                jax.ShapeDtypeStruct((heads, rows, 128), BF16),
                jax.ShapeDtypeStruct((rows, 128), BF16),
                jax.ShapeDtypeStruct((rows, 128), BF16),
                jax.ShapeDtypeStruct((batch, width), BF16),
                jax.ShapeDtypeStruct((batch, EARLY * BLOCK // 2), BF16),
            ),
            in_specs=[ANY, VM, VM, ANY, ANY, ANY, ANY, ANY],
            out_specs=(VM, VM, VM, ANY, VM),
            scratch_shapes=[
                pltpu.VMEM((batch, width), BF16),
                pltpu.VMEM((batch, width), BF16),
                pltpu.VMEM((SLOTS, width, BLOCK), BF16),
                pltpu.VMEM((6, batch, 128), BF16),
                pltpu.VMEM((batch, 128), F32),
                pltpu.VMEM((batch, 128), F32),
                dma, dma((SLOTS, 3)), dma, dma((PEERS,)), dma((PEERS,)),
            ],
            compiler_params=pltpu.CompilerParams(collective_id=0, has_side_effects=True, vmem_limit_bytes=LIMIT),
        )(tokens, lengths.reshape(batch, 1), norm_gain.reshape(1, width), w_query, w_key, w_value, w_gate, w_up)

        attended = pl.pallas_call(
            attend_kernel,
            name="attend",
            out_shape=jax.ShapeDtypeStruct((heads, rows, 128), BF16),
            in_specs=[SM, VM, VM, VM, ANY, ANY],
            out_specs=VM,
            scratch_shapes=[
                pltpu.VMEM((rows, heads, 128), F32),
                pltpu.VMEM((rows, heads, 128), F32),
                pltpu.VMEM((rows, 128), F32),
                pltpu.VMEM((rows, 128), F32),
                pltpu.VMEM((RING * ITEMS, CHUNK, 128), BF16),
                pltpu.VMEM((RING * ITEMS, CHUNK, 128), BF16),
                pltpu.SMEM((rows * (4096 // CHUNK) + ITEMS,), jnp.int32),
                pltpu.SMEM((rows * (4096 // CHUNK) + ITEMS,), jnp.int32),
                pltpu.VMEM((heads, 1), F32),
                pltpu.VMEM((heads, 1), F32),
                pltpu.VMEM((heads, 128), F32),
                dma((RING * ITEMS,)), dma((RING * ITEMS,)),
            ],
            compiler_params=pltpu.CompilerParams(vmem_limit_bytes=LIMIT),
        )(lengths, q_all, key_new, value_new, k_cache, v_cache)

        y = pl.pallas_call(
            combine_kernel,
            name="combine",
            out_shape=jax.ShapeDtypeStruct((batch, width), BF16),
            in_specs=[VM, ANY, ANY, ANY, ANY, ANY, ANY, ANY],
            out_specs=VM,
            scratch_shapes=[
                pltpu.VMEM((batch, width), BF16),
                pltpu.VMEM((batch, w_out.shape[0] + w_down.shape[0]), BF16),
                pltpu.VMEM((SLOTS, width, BLOCK), BF16),
                pltpu.VMEM((6, batch, 128), BF16),
                pltpu.VMEM((2, 16, width), BF16),
                pltpu.VMEM((n_chunks, batch, BLOCK), F32),
                pltpu.VMEM((n_chunks, 128, BLOCK), F32),
                pltpu.VMEM((n_chunks, 32, BLOCK), F32),
                pltpu.VMEM((n_chunks, 32, BLOCK), F32),
                pltpu.VMEM((n_chunks, 16, BLOCK), F32),
                pltpu.VMEM((n_chunks, 16, BLOCK), F32),
                dma, dma, dma((2,)), dma((SLOTS, 2)), dma((PEERS,)), dma((PEERS,)),
                dma((10, n_chunks)), dma((10, n_chunks)),
            ],
            compiler_params=pltpu.CompilerParams(collective_id=1, has_side_effects=True, vmem_limit_bytes=LIMIT),
        )(attended, tokens, normed, early, w_gate, w_up, w_out, w_down)
        return y, key_new.reshape(rows, 1, 128), value_new.reshape(rows, 1, 128)

    in_specs = (P('replica', None), P('replica'), P('replica', None, None, None), P('replica', None, None, None), P(None), P(None, 'model'), P(None, None), P(None, None), P('model', None), P(None, 'model'), P(None, 'model'), P('model', None))
    out_specs = (P('replica', None), P(('replica', 'model'), None, None), P(('replica', 'model'), None, None))
    return jax.shard_map(local_step, mesh=mesh, in_specs=in_specs, out_specs=out_specs, check_vma=False)
```

```python
import functools
import math
import jax
import jax.numpy as jnp
from jax import lax
from jax.experimental import pallas as pl
from jax.experimental.pallas import tpu as pltpu
from jax.sharding import PartitionSpec as P

ROPE_BASE = 10000.0
NORM_EPS = 1e-6
MASK_VALUE = -1e30
BF16, F32 = jnp.bfloat16, jnp.float32
MESH = pl.DeviceIdType.MESH

PEERS = 8
SLOTS = 4
BLOCK = 512
EARLY = 4
CHUNK = 512
ITEMS = 4
RING = 3
CHUNK_COLS = 512
LAGS = (0, 1, 4, 10, 14, 18, 19)


def greet(me):
    barrier = pltpu.get_barrier_semaphore()
    for step in range(1, PEERS):
        peer = lax.rem(me + step, PEERS)
        pl.semaphore_signal(barrier, inc=1, device_id={"model": peer}, device_id_type=MESH)
    return barrier


def gate_up_copies(block, slot, gate_hbm, up_hbm, ring, sems):
    half = BLOCK // 2
    columns = pl.ds(pl.multiple_of(block * half, half), half)
    return (
        pltpu.make_async_copy(gate_hbm.at[:, columns], ring.at[slot, :, pl.ds(0, half)], sems.at[slot, 0]),
        pltpu.make_async_copy(up_hbm.at[:, columns], ring.at[slot, :, pl.ds(half, half)], sems.at[slot, 1]),
    )


def hidden_block(normed, weights):
    half = BLOCK // 2
    both = jnp.dot(normed, weights, preferred_element_type=F32)
    gate, up = both[:, :half], both[:, half:]
    return (gate * lax.logistic(gate) * up).astype(BF16)


def rope(values, cos_part, sin_part):
    return values * cos_part + pltpu.roll(values, 64, 1) * sin_part


def project_kernel(x_hbm, lengths_hbm, gain_hbm, wq_hbm, wk_hbm, wv_hbm, gate_hbm, up_hbm,
                   q_out, knew_ref, vnew_ref, normed, hidden_ref,
                   x_ref, lengths_ref, gain_ref, ring, q_scr, cos_scr, sin_scr, stat_scr, gain_scr, x_sem, in_sem, sems, send_sem, recv_sem):
    me = lax.axis_index("model")
    batch = x_ref.shape[0]
    width = x_ref.shape[1]
    rows = batch // PEERS
    barrier = greet(me)
    x_copy = pltpu.make_async_copy(x_hbm, x_ref, x_sem)
    l_copy = pltpu.make_async_copy(lengths_hbm, lengths_ref, in_sem.at[0])
    g_copy = pltpu.make_async_copy(gain_hbm, gain_ref, in_sem.at[1])
    for copy in (l_copy, x_copy, g_copy):
        copy.start()
    first = (pltpu.make_async_copy(wq_hbm.at[:, pl.ds(0, 512)], ring.at[0], sems.at[0, 0]),)
    second = (
        pltpu.make_async_copy(wq_hbm.at[:, pl.ds(512, 256)], ring.at[1, :, pl.ds(0, 256)], sems.at[1, 0]),
        pltpu.make_async_copy(wk_hbm, ring.at[1, :, pl.ds(256, 128)], sems.at[1, 1]),
        pltpu.make_async_copy(wv_hbm, ring.at[1, :, pl.ds(384, 128)], sems.at[1, 2]),
    )
    gu = lambda block, slot: gate_up_copies(block, slot, gate_hbm, up_hbm, ring, sems)

    hb = batch // 2
    l_copy.wait()
    spread = jnp.broadcast_to(lengths_ref[...].astype(F32).reshape(1, batch), (128, batch)).T
    lane = lax.broadcasted_iota(jnp.int32, (hb, 128), 1)
    low = lane < 64
    pair = jnp.where(low, lane, lane - 64).astype(F32)
    inv_freq = jnp.exp(pair * (-2.0 * math.log(ROPE_BASE) / 128))
    angles = jnp.where(low, spread[:hb], spread[hb:]) * inv_freq
    cos_part, sin_part = jnp.cos(angles), jnp.sin(angles)
    cos_turn, sin_turn = pltpu.roll(cos_part, 64, 1), pltpu.roll(sin_part, 64, 1)
    cos_scr[:hb] = jnp.where(low, cos_part, cos_turn)
    cos_scr[hb:] = jnp.where(low, cos_turn, cos_part)
    sin_scr[:hb] = jnp.where(low, -sin_part, sin_turn)
    sin_scr[hb:] = jnp.where(low, -sin_turn, sin_part)

    x_copy.wait()
    for copy in first:
        copy.start()
    tiles = width // 128

    def square_rows(r, _):
        at = pl.ds(pl.multiple_of(r * 16, 16), 16)
        sums = [jnp.zeros((16, 128), F32) for _ in range(4)]
        for j in range(tiles):
            values = x_ref[at, j * 128:(j + 1) * 128].astype(F32)
            sums[j % 4] = sums[j % 4] + values * values
        stat_scr[at, :] = (sums[0] + sums[1]) + (sums[2] + sums[3])
        return 0

    lax.fori_loop(0, batch // 16, square_rows, 0)
    mean_sq = jnp.sum(stat_scr[...], axis=-1, keepdims=True) * (1.0 / width)
    stat_scr[...] = jnp.broadcast_to(lax.rsqrt(mean_sq + NORM_EPS), (batch, 128))

    def norm_rows(r, _):
        at = pl.ds(pl.multiple_of(r * 16, 16), 16)
        factor = stat_scr[at, :]
        for j in range(tiles):
            cols = slice(j * 128, (j + 1) * 128)
            normed[at, cols] = (x_ref[at, cols].astype(F32) * factor * gain_scr[:, cols]).astype(BF16)
        return 0

    for copy in second:
        copy.start()
    g_copy.wait()
    gain_scr[...] = gain_ref[...].astype(F32).reshape(1, width)
    lax.fori_loop(0, batch // 16, norm_rows, 0)

    for copy in first:
        copy.wait()
    for copy in gu(0, 2):
        copy.start()
    head4 = jnp.dot(normed[...], ring[0], preferred_element_type=F32)
    for h in range(4):
        q_scr[h] = rope(head4[:, h * 128:(h + 1) * 128], cos_scr[...], sin_scr[...]).astype(BF16)
    for copy in second:
        copy.wait()
    for copy in gu(1, 3) + gu(2, 0):
        copy.start()
    tail = jnp.dot(normed[...], ring[1], preferred_element_type=F32)
    for h in range(2):
        q_scr[4 + h] = rope(tail[:, h * 128:(h + 1) * 128], cos_scr[...], sin_scr[...]).astype(BF16)
    k_all = rope(tail[:, 256:384], cos_scr[...], sin_scr[...])
    cos_scr[...] = k_all
    sin_scr[...] = tail[:, 384:512]
    mine = pl.ds(pl.multiple_of(me * rows, rows), rows)
    knew_ref[...] = cos_scr[mine, :].astype(BF16)
    vnew_ref[...] = sin_scr[mine, :].astype(BF16)
    for copy in gu(3, 1):
        copy.start()

    pl.semaphore_wait(barrier, PEERS - 1)
    heads = pl.ds(me * 6, 6)
    sends = []
    for step in range(1, PEERS):
        peer = lax.rem(me + step, PEERS)
        sends.append(pltpu.make_async_remote_copy(
            src_ref=q_scr.at[:, pl.ds(pl.multiple_of(peer * rows, rows), rows), :],
            dst_ref=q_out.at[heads],
            send_sem=send_sem.at[step], recv_sem=recv_sem.at[step],
            device_id={"model": peer}, device_id_type=MESH))
        sends[-1].start()
    q_out[heads] = q_scr[:, mine, :]

    half = BLOCK // 2

    def block_step(n, _):
        slot = lax.rem(n + 2, SLOTS)
        for copy in gu(n, slot):
            copy.wait()
        hidden_ref[:, pl.ds(pl.multiple_of(n * half, half), half)] = hidden_block(normed[...], ring[slot])

        @pl.when(n + SLOTS < EARLY)
        def _():
            for copy in gu(n + SLOTS, slot):
                copy.start()
        return 0

    lax.fori_loop(0, EARLY, block_step, 0)
    for copy in sends:
        copy.wait()


def attend_kernel(lengths_ref, q_in, k16, v16, k_hbm, v_hbm, o_ref, key_out, value_out,
                  q_scr, o_scr, k_scr, v_scr, k_buf, v_buf, item_row, item_chunk, m_run, l_run, acc_run,
                  k_sem, v_sem, out_sem):
    me = lax.axis_index("model")
    rows = o_ref.shape[1]
    head_count = o_ref.shape[0]
    context = k_hbm.shape[2]
    base = me * rows
    scale = 128 ** -0.5
    def chunks_of(b):
        return lax.div(lengths_ref[base + b] + (CHUNK - 1), CHUNK)

    total = chunks_of(0)
    for b in range(1, rows):
        total = total + chunks_of(b)
    bodies = lax.div(total + (ITEMS - 1), ITEMS)

    def copies(g, j):
        n = g * ITEMS + j
        start = pl.multiple_of(jnp.minimum(item_chunk[n] * CHUNK, context - CHUNK), CHUNK)
        row = base + item_row[n]
        slot = lax.rem(g, RING) * (ITEMS // 2) + j // 2
        sem = lax.rem(g, RING) * ITEMS + j
        src, lanes = pl.ds(start, CHUNK), pl.ds(128 * (j % 2), 128)
        return (pltpu.make_async_copy(k_hbm.at[row, 0, src, :], k_buf.at[slot, :, lanes], k_sem.at[sem]),
                pltpu.make_async_copy(v_hbm.at[row, 0, src, :], v_buf.at[slot, :, lanes], v_sem.at[sem]))

    def launch(g, state):
        b, c = state
        for j in range(ITEMS):
            n = g * ITEMS + j
            item_row[n] = b
            item_chunk[n] = c
            turn = (c + 1 >= chunks_of(b)) & (b < rows - 1)
            b, c = jnp.where(turn, b + 1, b), jnp.where(turn, 0, c + 1)

        @pl.when(g < bodies)
        def _():
            for j in range(ITEMS):
                for copy in copies(g, j):
                    copy.start()
        return b, c

    state = (jnp.int32(0), jnp.int32(0))
    for g in range(RING - 1):
        state = launch(g, state)

    outputs = [pltpu.make_async_copy(k16, key_out, out_sem.at[0]), pltpu.make_async_copy(v16, value_out, out_sem.at[1])]
    for copy in outputs:
        copy.start()
    k_scr[...] = k16[...].astype(F32)
    v_scr[...] = v16[...].astype(F32)
    q_scr[...] = jnp.swapaxes(q_in[...].astype(F32), 0, 1).astype(BF16)
    m_run[...] = jnp.zeros_like(m_run)
    l_run[...] = jnp.ones_like(l_run)
    acc_run[...] = jnp.zeros_like(acc_run)

    def body(g, state):
        state = launch(g + RING - 1, state)
        for j in range(ITEMS):
            for copy in copies(g, j):
                copy.wait()
        m, l, acc = m_run[...], l_run[...], acc_run[...]
        blank = jnp.zeros((head_count, 128), BF16)
        scored = []
        for p in range(ITEMS // 2):
            slot = lax.rem(g, RING) * (ITEMS // 2) + p
            news, q_rows = [], []
            for j in range(2):
                n = g * ITEMS + 2 * p + j
                b, c = item_row[n], item_chunk[n]
                q16 = q_scr[b]
                q32 = q16.astype(F32)
                q_rows.append(jnp.concatenate([q16, blank] if j == 0 else [blank, q16], axis=1))
                s_new = jnp.sum(q32 * k_scr[pl.ds(b, 1), :], axis=-1, keepdims=True) * scale
                news.append((b, c, s_new, lengths_ref[base + b] - c * CHUNK))
            s_pair = lax.dot_general(jnp.concatenate(q_rows, axis=0), k_buf[slot], (((1,), (1,)), ((), ())), preferred_element_type=F32) * scale
            for j in range(2):
                b, c, s_new, left = news[j]
                s = s_pair[j * head_count:(j + 1) * head_count]
                s = jnp.where(lax.broadcasted_iota(jnp.int32, s.shape, 1) < left, s, MASK_VALUE)
                scored.append((s, jnp.max(s, axis=-1, keepdims=True), s_new, b, c))
        for p in range(ITEMS // 2):
            slot = lax.rem(g, RING) * (ITEMS // 2) + p
            tops, weights, shrinks = [], [], []
            for j in range(2):
                s, s_max, s_new, b, c = scored[2 * p + j]
                m_prev = jnp.where(c == 0, s_new, m)
                m = jnp.maximum(m_prev, s_max)
                e = jnp.exp(s - m)
                shrink = jnp.exp(m_prev - m)
                l = jnp.where(c == 0, 1.0, l) * shrink + jnp.sum(e, axis=-1, keepdims=True)
                tops.append(l)
                shrinks.append(shrink)
                weights.append(e.astype(BF16))
            mixed = jnp.dot(jnp.concatenate(weights, axis=0), v_buf[slot], preferred_element_type=F32)
            for j in range(2):
                _, _, _, b, c = scored[2 * p + j]
                part = mixed[j * head_count:(j + 1) * head_count, j * 128:(j + 1) * 128]
                acc = jnp.where(c == 0, v_scr[pl.ds(b, 1), :], acc) * shrinks[j] + part
                o_scr[b] = acc / tops[j]
        m_run[...], l_run[...], acc_run[...] = m, l, acc
        return state

    lax.fori_loop(0, bodies, body, state)
    for copy in outputs:
        copy.wait()
    o_ref[...] = jnp.swapaxes(o_scr[...], 0, 1).astype(BF16)


def combine_kernel(o_ref, x_hbm, normed, early_ref, gate_hbm, up_hbm, wo_hbm, wd_hbm, y_ref,
                   act, ring, o_full, x_rows, part, pair_in, in1x, in1y, in2x, in2y,
                   x_sem, sems, o_send, o_recv, c_send, c_recv):
    me = lax.axis_index("model")
    core = lax.rem(me, 2)
    xi = lax.rem(lax.div(me, 2), 2)
    yi = lax.div(me, 4)
    partner = me + 1 - 2 * core
    x_peer = me + 2 - 4 * xi
    y_peer = me + 4 - 8 * yi
    batch = normed.shape[0]
    rows = batch // PEERS
    late = gate_hbm.shape[1] // (BLOCK // 2) - EARLY
    n_chunks = y_ref.shape[1] // CHUNK_COLS
    o_width = wo_hbm.shape[0]
    f_width = wd_hbm.shape[0]
    half = BLOCK // 2
    barrier = greet(me)

    early_width = EARLY * half

    def gu(n, slot):
        return gate_up_copies(n + EARLY, slot, gate_hbm, up_hbm, ring, sems)

    def down(t, slot):
        columns = pl.ds(pl.multiple_of(t * CHUNK_COLS, CHUNK_COLS), CHUNK_COLS)
        lanes = pl.ds(0, CHUNK_COLS)
        return (
            pltpu.make_async_copy(wo_hbm.at[:, columns], ring.at[slot, pl.ds(0, o_width), lanes], sems.at[slot, 0]),
            pltpu.make_async_copy(wd_hbm.at[:, columns], ring.at[slot, pl.ds(o_width, f_width), lanes], sems.at[slot, 1]),
        )

    def fetch(n):
        slot = lax.rem(n, SLOTS)

        @pl.when(n < late)
        def _():
            for copy in gu(n, slot):
                copy.start()

        @pl.when((n >= late) & (n < late + n_chunks))
        def _():
            for copy in down(n - late, slot):
                copy.start()

    for copy in gu(0, 0):
        copy.start()
    row_x = core * 128 + xi * 32 + yi * 16
    row_y = core * 128 + 64 + yi * 32 + xi * 16
    x_copies = []
    for k, row in enumerate((row_x, row_y)):
        x_copies.append(pltpu.make_async_copy(x_hbm.at[pl.ds(pl.multiple_of(row, 16), 16), :], x_rows.at[k], x_sem.at[k]))
    pl.semaphore_wait(barrier, PEERS - 1)
    mine = pl.ds(pl.multiple_of(me * rows, rows), rows)
    sends = []
    for step in range(1, PEERS):
        peer = lax.rem(me + step, PEERS)
        sends.append(pltpu.make_async_remote_copy(
            src_ref=o_ref.at[pl.ds(peer * 6, 6)], dst_ref=o_full.at[:, mine, :],
            send_sem=o_send.at[step], recv_sem=o_recv.at[step],
            device_id={"model": peer}, device_id_type=MESH))
        sends[-1].start()
    o_full[:, mine, :] = o_ref[pl.ds(me * 6, 6)]
    act[:, o_width:o_width + early_width] = early_ref[...]
    for copy in gu(1, 1):
        copy.start()

    def block_step(n, _):
        slot = lax.rem(n, SLOTS)
        for copy in gu(n, slot):
            copy.wait()

        @pl.when(n == 0)
        def _():
            fetch(2)
            fetch(3)
        at = pl.ds(pl.multiple_of(o_width + early_width + n * half, half), half)
        act[:, at] = hidden_block(normed[...], ring[slot])
        fetch(n + SLOTS)
        return 0

    lax.fori_loop(0, late - 1, block_step, 0)
    for copy in x_copies:
        copy.start()
    block_step(late - 1, 0)
    for copy in x_copies:
        copy.wait()
    for copy in sends:
        copy.wait()
    for h in range(6):
        act[:, h * 128:(h + 1) * 128] = o_full[h]

    my_half = pl.multiple_of(core * 128, 128)
    other_half = pl.multiple_of(128 - core * 128, 128)
    keep1x = pl.multiple_of(my_half + xi * 32, 32)
    give1x = pl.multiple_of(my_half + 32 - xi * 32, 32)
    keep1y = pl.multiple_of(my_half + 64 + yi * 32, 32)
    give1y = pl.multiple_of(my_half + 96 - yi * 32, 32)
    keep2x = pl.multiple_of(keep1x + yi * 16, 16)
    give2x = pl.multiple_of(keep1x + 16 - yi * 16, 16)
    keep2y = pl.multiple_of(keep1y + xi * 16, 16)
    give2y = pl.multiple_of(keep1y + 16 - xi * 16, 16)

    def cols(t):
        return pl.ds(pl.multiple_of(t * CHUNK_COLS, CHUNK_COLS), CHUNK_COLS)

    def remote(kind, t, src, dst, peer):
        return pltpu.make_async_remote_copy(
            src_ref=src, dst_ref=dst, send_sem=c_send.at[kind, t], recv_sem=c_recv.at[kind, t],
            device_id={"model": peer}, device_id_type=MESH)

    def pair_sum(t):
        return remote(0, t, part.at[t, pl.ds(other_half, 128), :], pair_in.at[t], partner)

    def scatter1(t):
        return (remote(1, t, part.at[t, pl.ds(give1x, 32), :], in1x.at[t], x_peer),
                remote(2, t, part.at[t, pl.ds(give1y, 32), :], in1y.at[t], y_peer))

    def scatter2(t):
        return (remote(3, t, part.at[t, pl.ds(give2x, 16), :], in2x.at[t], y_peer),
                remote(4, t, part.at[t, pl.ds(give2y, 16), :], in2y.at[t], x_peer))

    def spread(kind, t, row, count, peer):
        at = y_ref.at[pl.ds(row, count), cols(t)]
        return remote(kind, t, at, at, peer)

    def gather1(t):
        return spread(5, t, keep2x, 16, y_peer), spread(6, t, keep2y, 16, x_peer)

    def gather2(t):
        return spread(7, t, keep1x, 32, x_peer), spread(8, t, keep1y, 32, y_peer)

    def pair_copy(t):
        return (spread(9, t, my_half, 128, partner),)

    def start(copies):
        for copy in copies:
            copy.start()

    def arrive(copies):
        for copy in copies:
            copy.wait_recv()

    def stage_compute(t):
        slot = lax.rem(t + late, SLOTS)
        for copy in down(t, slot):
            copy.wait()
        part[t] = jnp.dot(act[...], ring[slot, pl.ds(0, o_width + f_width), pl.ds(0, CHUNK_COLS)], preferred_element_type=F32)
        pair_sum(t).start()
        fetch(t + late + SLOTS)

    def stage_scatter1(t):
        pair_sum(t).wait_recv()
        part[t, pl.ds(my_half, 128), :] = part[t, pl.ds(my_half, 128), :] + pair_in[t]
        start(scatter1(t))

    def stage_scatter2(t):
        arrive(scatter1(t))
        part[t, pl.ds(keep1x, 32), :] = part[t, pl.ds(keep1x, 32), :] + in1x[t]
        part[t, pl.ds(keep1y, 32), :] = part[t, pl.ds(keep1y, 32), :] + in1y[t]
        start(scatter2(t))

    def stage_gather1(t):
        arrive(scatter2(t))
        for k, (keep, inbox) in enumerate(((keep2x, in2x), (keep2y, in2y))):
            total = part[t, pl.ds(keep, 16), :] + inbox[t]
            y_ref[pl.ds(keep, 16), cols(t)] = (x_rows[k, :, cols(t)].astype(F32) + total).astype(BF16)
        start(gather1(t))

    def stage_gather2(t):
        arrive(gather1(t))
        start(gather2(t))

    def stage_pair(t):
        arrive(gather2(t))
        start(pair_copy(t))

    def stage_end(t):
        arrive(pair_copy(t))

    stages = (stage_compute, stage_scatter1, stage_scatter2, stage_gather1, stage_gather2, stage_pair, stage_end)

    def iteration(i, _):
        for lag, stage in zip(LAGS, stages):
            t = i - lag

            @pl.when((t >= 0) & (t < n_chunks))
            def _(stage=stage, t=t):
                stage(t)
        return 0

    lax.fori_loop(0, n_chunks + LAGS[-1], iteration, 0)

    def drain(t, _):
        for copy in (pair_sum(t),) + scatter1(t) + scatter2(t) + gather1(t) + gather2(t) + pair_copy(t):
            copy.wait_send()
        return 0

    lax.fori_loop(0, n_chunks, drain, 0)


ANY = pl.BlockSpec(memory_space=pltpu.HBM)
VM = pl.BlockSpec(memory_space=pltpu.VMEM)
SM = pl.BlockSpec(memory_space=pltpu.SMEM)
LIMIT = 50 << 20


def project_call(tokens, lengths, norm_gain, w_query, w_key, w_value, w_gate, w_up):
    lengths, norm_gain = (pltpu.with_memory_space_constraint(a, pltpu.HBM) for a in (lengths, norm_gain))
    batch, width = tokens.shape
    rows = batch // PEERS
    dma = pltpu.SemaphoreType.DMA
    return pl.pallas_call(
        project_kernel,
        name="project",
        out_shape=(
            pltpu.VMEM((width // 128, rows, 128), BF16),
            pltpu.VMEM((rows, 128), BF16),
            pltpu.VMEM((rows, 128), BF16),
            pltpu.VMEM((batch, width), BF16),
            pltpu.VMEM((batch, EARLY * BLOCK // 2), BF16),
        ),
        in_specs=[ANY, ANY, ANY, ANY, ANY, ANY, ANY, ANY],
        out_specs=(VM, VM, VM, VM, VM),
        scratch_shapes=[
            pltpu.VMEM((batch, width), BF16),
            pltpu.VMEM((batch,), jnp.int32),
            pltpu.VMEM((width,), BF16),
            pltpu.VMEM((SLOTS, width, BLOCK), BF16),
            pltpu.VMEM((6, batch, 128), BF16),
            pltpu.VMEM((batch, 128), F32),
            pltpu.VMEM((batch, 128), F32),
            pltpu.VMEM((batch, 128), F32),
            pltpu.VMEM((1, width), F32),
            dma, dma((2,)), dma((SLOTS, 3)), dma((PEERS,)), dma((PEERS,)),
        ],
        compiler_params=pltpu.CompilerParams(collective_id=0, has_side_effects=True, vmem_limit_bytes=LIMIT),
    )(tokens, lengths, norm_gain, w_query, w_key, w_value, w_gate, w_up)


def attend_call(lengths, q_all, key_new, value_new, k_cache, v_cache):
    heads, rows, _ = q_all.shape
    dma = pltpu.SemaphoreType.DMA
    return pl.pallas_call(
        attend_kernel,
        name="attend",
        out_shape=(
            pltpu.VMEM((heads, rows, 128), BF16),
            jax.ShapeDtypeStruct((rows, 128), BF16),
            jax.ShapeDtypeStruct((rows, 128), BF16),
        ),
        in_specs=[SM, VM, VM, VM, ANY, ANY],
        out_specs=(VM, ANY, ANY),
        scratch_shapes=[
            pltpu.VMEM((rows, heads, 128), BF16),
            pltpu.VMEM((rows, heads, 128), F32),
            pltpu.VMEM((rows, 128), F32),
            pltpu.VMEM((rows, 128), F32),
            pltpu.VMEM((RING * ITEMS // 2, CHUNK, 256), BF16),
            pltpu.VMEM((RING * ITEMS // 2, CHUNK, 256), BF16),
            pltpu.SMEM((rows * (k_cache.shape[2] // CHUNK) + RING * ITEMS,), jnp.int32),
            pltpu.SMEM((rows * (k_cache.shape[2] // CHUNK) + RING * ITEMS,), jnp.int32),
            pltpu.VMEM((heads, 1), F32),
            pltpu.VMEM((heads, 1), F32),
            pltpu.VMEM((heads, 128), F32),
            dma((RING * ITEMS,)), dma((RING * ITEMS,)), dma((2,)),
        ],
        compiler_params=pltpu.CompilerParams(vmem_limit_bytes=20 << 20),
    )(lengths, q_all, key_new, value_new, k_cache, v_cache)


def combine_call(attended, tokens, normed, early, w_gate, w_up, w_out, w_down):
    attended, normed, early = (pltpu.with_memory_space_constraint(a, pltpu.VMEM) for a in (attended, normed, early))
    batch, width = tokens.shape
    n_chunks = width // CHUNK_COLS
    dma = pltpu.SemaphoreType.DMA
    return pl.pallas_call(
        combine_kernel,
        name="combine",
        out_shape=pltpu.VMEM((batch, width), BF16),
        in_specs=[VM, ANY, VM, VM, ANY, ANY, ANY, ANY],
        out_specs=VM,
        scratch_shapes=[
            pltpu.VMEM((batch, w_out.shape[0] + w_down.shape[0]), BF16),
            pltpu.VMEM((SLOTS, width, BLOCK), BF16),
            pltpu.VMEM((6, batch, 128), BF16),
            pltpu.VMEM((2, 16, width), BF16),
            pltpu.VMEM((n_chunks, batch, CHUNK_COLS), F32),
            pltpu.VMEM((n_chunks, 128, CHUNK_COLS), F32),
            pltpu.VMEM((n_chunks, 32, CHUNK_COLS), F32),
            pltpu.VMEM((n_chunks, 32, CHUNK_COLS), F32),
            pltpu.VMEM((n_chunks, 16, CHUNK_COLS), F32),
            pltpu.VMEM((n_chunks, 16, CHUNK_COLS), F32),
            dma((2,)), dma((SLOTS, 2)), dma((PEERS,)), dma((PEERS,)),
            dma((10, n_chunks)), dma((10, n_chunks)),
        ],
        compiler_params=pltpu.CompilerParams(collective_id=1, has_side_effects=True, vmem_limit_bytes=LIMIT),
    )(attended, tokens, normed, early, w_gate, w_up, w_out, w_down)


def solution(mesh):
    def local_step(tokens, lengths, k_cache, v_cache, norm_gain, w_query, w_key, w_value, w_out, w_gate, w_up, w_down):
        rows = tokens.shape[0] // PEERS
        q_all, key_new, value_new, normed, early = project_call(tokens, lengths, norm_gain, w_query, w_key, w_value, w_gate, w_up)
        attended, key_new, value_new = attend_call(lengths, q_all, key_new, value_new, k_cache, v_cache)
        y = combine_call(attended, tokens, normed, early, w_gate, w_up, w_out, w_down)
        return y, key_new.reshape(rows, 1, 128), value_new.reshape(rows, 1, 128)

    in_specs = (P('replica', None), P('replica'), P('replica', None, None, None), P('replica', None, None, None), P(None), P(None, 'model'), P(None, None), P(None, None), P('model', None), P(None, 'model'), P(None, 'model'), P('model', None))
    out_specs = (P('replica', None), P(('replica', 'model'), None, None), P(('replica', 'model'), None, None))
    return jax.shard_map(local_step, mesh=mesh, in_specs=in_specs, out_specs=out_specs, check_vma=False)
```

```python
import functools
import math
import jax
import jax.numpy as jnp
from jax import lax
from jax.experimental import pallas as pl
from jax.experimental.pallas import tpu as pltpu
from jax.sharding import PartitionSpec as P

ROPE_BASE = 10000.0
NORM_EPS = 1e-6
MASK_VALUE = -1e30
BF16, F32 = jnp.bfloat16, jnp.float32
MESH = pl.DeviceIdType.MESH

PEERS = 8
SLOTS = 4
BLOCK = 512
EARLY = 4
CHUNK = 512
ITEMS = 8
PIECES = 12
PIECE_STEP = 2
AHEAD = 2
C_SLOTS = 3
RING = 4
CHUNK_COLS = 512
LAGS = (0, 1, 4, 10, 14, 18, 19)


def greet(me):
    barrier = pltpu.get_barrier_semaphore()
    for step in range(1, PEERS):
        peer = lax.rem(me + step, PEERS)
        pl.semaphore_signal(barrier, inc=1, device_id={"model": peer}, device_id_type=MESH)
    return barrier


def gate_up_copies(block, slot, gate_hbm, up_hbm, ring, sems):
    half = BLOCK // 2
    columns = pl.ds(pl.multiple_of(block * half, half), half)
    return (
        pltpu.make_async_copy(gate_hbm.at[:, columns], ring.at[slot, :, pl.ds(0, half)], sems.at[slot, 0]),
        pltpu.make_async_copy(up_hbm.at[:, columns], ring.at[slot, :, pl.ds(half, half)], sems.at[slot, 1]),
    )


def hidden_block(normed, weights):
    half = BLOCK // 2
    both = jnp.dot(normed, weights, preferred_element_type=F32)
    gate, up = both[:, :half], both[:, half:]
    return (gate * lax.logistic(gate) * up).astype(BF16)


def rope(values, cos_part, sin_part):
    return values * cos_part + pltpu.roll(values, 64, 1) * sin_part


def project_kernel(x_hbm, lengths_hbm, gain_hbm, wq_hbm, wk_hbm, wv_hbm, gate_hbm, up_hbm,
                   q_out, knew_ref, vnew_ref, normed, hidden_ref,
                   x_ref, lengths_ref, gain_ref, ring, q_scr, cos_scr, sin_scr, stat_scr, gain_scr, x_sem, in_sem, sems, send_sem, recv_sem):
    me = lax.axis_index("model")
    batch = x_ref.shape[0]
    width = x_ref.shape[1]
    rows = batch // PEERS
    barrier = greet(me)
    x_copy = pltpu.make_async_copy(x_hbm, x_ref, x_sem)
    l_copy = pltpu.make_async_copy(lengths_hbm, lengths_ref, in_sem.at[0])
    g_copy = pltpu.make_async_copy(gain_hbm, gain_ref, in_sem.at[1])
    for copy in (l_copy, x_copy, g_copy):
        copy.start()
    first = (pltpu.make_async_copy(wq_hbm.at[:, pl.ds(0, 512)], ring.at[0], sems.at[0, 0]),)
    second = (
        pltpu.make_async_copy(wq_hbm.at[:, pl.ds(512, 256)], ring.at[1, :, pl.ds(0, 256)], sems.at[1, 0]),
        pltpu.make_async_copy(wk_hbm, ring.at[1, :, pl.ds(256, 128)], sems.at[1, 1]),
        pltpu.make_async_copy(wv_hbm, ring.at[1, :, pl.ds(384, 128)], sems.at[1, 2]),
    )
    gu = lambda block, slot: gate_up_copies(block, slot, gate_hbm, up_hbm, ring, sems)

    hb = batch // 2
    l_copy.wait()
    spread = jnp.broadcast_to(lengths_ref[...].astype(F32).reshape(1, batch), (128, batch)).T
    lane = lax.broadcasted_iota(jnp.int32, (hb, 128), 1)
    low = lane < 64
    pair = jnp.where(low, lane, lane - 64).astype(F32)
    inv_freq = jnp.exp(pair * (-2.0 * math.log(ROPE_BASE) / 128))
    angles = jnp.where(low, spread[:hb], spread[hb:]) * inv_freq
    cos_part, sin_part = jnp.cos(angles), jnp.sin(angles)
    cos_turn, sin_turn = pltpu.roll(cos_part, 64, 1), pltpu.roll(sin_part, 64, 1)
    cos_scr[:hb] = jnp.where(low, cos_part, cos_turn)
    cos_scr[hb:] = jnp.where(low, cos_turn, cos_part)
    sin_scr[:hb] = jnp.where(low, -sin_part, sin_turn)
    sin_scr[hb:] = jnp.where(low, -sin_turn, sin_part)

    x_copy.wait()
    for copy in first:
        copy.start()
    tiles = width // 128

    def square_rows(r, _):
        at = pl.ds(pl.multiple_of(r * 16, 16), 16)
        sums = [jnp.zeros((16, 128), F32) for _ in range(4)]
        for j in range(tiles):
            values = x_ref[at, j * 128:(j + 1) * 128].astype(F32)
            sums[j % 4] = sums[j % 4] + values * values
        stat_scr[at, :] = (sums[0] + sums[1]) + (sums[2] + sums[3])
        return 0

    lax.fori_loop(0, batch // 16, square_rows, 0)
    mean_sq = jnp.sum(stat_scr[...], axis=-1, keepdims=True) * (1.0 / width)
    stat_scr[...] = jnp.broadcast_to(lax.rsqrt(mean_sq + NORM_EPS), (batch, 128))

    def norm_rows(r, _):
        at = pl.ds(pl.multiple_of(r * 16, 16), 16)
        factor = stat_scr[at, :]
        for j in range(tiles):
            cols = slice(j * 128, (j + 1) * 128)
            normed[at, cols] = (x_ref[at, cols].astype(F32) * factor * gain_scr[:, cols]).astype(BF16)
        return 0

    for copy in second:
        copy.start()
    g_copy.wait()
    gain_scr[...] = gain_ref[...].astype(F32).reshape(1, width)
    lax.fori_loop(0, batch // 16, norm_rows, 0)

    for copy in first:
        copy.wait()
    for copy in gu(0, 2):
        copy.start()
    head4 = jnp.dot(normed[...], ring[0], preferred_element_type=F32)
    for h in range(4):
        q_scr[h] = rope(head4[:, h * 128:(h + 1) * 128], cos_scr[...], sin_scr[...]).astype(BF16)
    for copy in second:
        copy.wait()
    for copy in gu(1, 3) + gu(2, 0):
        copy.start()
    tail = jnp.dot(normed[...], ring[1], preferred_element_type=F32)
    for h in range(2):
        q_scr[4 + h] = rope(tail[:, h * 128:(h + 1) * 128], cos_scr[...], sin_scr[...]).astype(BF16)
    k_all = rope(tail[:, 256:384], cos_scr[...], sin_scr[...])
    cos_scr[...] = k_all
    sin_scr[...] = tail[:, 384:512]
    mine = pl.ds(pl.multiple_of(me * rows, rows), rows)
    knew_ref[...] = cos_scr[mine, :].astype(BF16)
    vnew_ref[...] = sin_scr[mine, :].astype(BF16)
    for copy in gu(3, 1):
        copy.start()

    pl.semaphore_wait(barrier, PEERS - 1)
    heads = pl.ds(me * 6, 6)
    sends = []
    for step in range(1, PEERS):
        peer = lax.rem(me + step, PEERS)
        sends.append(pltpu.make_async_remote_copy(
            src_ref=q_scr.at[:, pl.ds(pl.multiple_of(peer * rows, rows), rows), :],
            dst_ref=q_out.at[heads],
            send_sem=send_sem.at[step], recv_sem=recv_sem.at[step],
            device_id={"model": peer}, device_id_type=MESH))
        sends[-1].start()
    q_out[heads] = q_scr[:, mine, :]

    half = BLOCK // 2

    def block_step(n, _):
        slot = lax.rem(n + 2, SLOTS)
        for copy in gu(n, slot):
            copy.wait()
        hidden_ref[:, pl.ds(pl.multiple_of(n * half, half), half)] = hidden_block(normed[...], ring[slot])

        @pl.when(n + SLOTS < EARLY)
        def _():
            for copy in gu(n + SLOTS, slot):
                copy.start()
        return 0

    lax.fori_loop(0, EARLY, block_step, 0)
    for copy in sends:
        copy.wait()


def attend_kernel(lengths_ref, q_in, k16, v16, k_hbm, v_hbm, gate_hbm, up_hbm, o_ref, key_out, value_out, ahead_ref,
                  q_scr, o_scr, k_scr, v_scr, s_scr, top_scr, new_scr, k_buf, v_buf, item_row, item_chunk, m_run, l_run, acc_run,
                  k_sem, v_sem, out_sem, a_sem):
    me = lax.axis_index("model")
    rows = o_ref.shape[1]
    head_count = o_ref.shape[0]
    context = k_hbm.shape[2]
    base = me * rows
    scale = 128 ** -0.5
    def chunks_of(b):
        return lax.div(lengths_ref[base + b] + (CHUNK - 1), CHUNK)

    total = chunks_of(0)
    for b in range(1, rows):
        total = total + chunks_of(b)
    bodies = lax.div(total + (ITEMS - 1), ITEMS)

    def copies(g, j):
        n = g * ITEMS + j
        start = pl.multiple_of(jnp.minimum(item_chunk[n] * CHUNK, context - CHUNK), CHUNK)
        row = base + item_row[n]
        slot = lax.rem(g, RING) * (ITEMS // 2) + j // 2
        sem = lax.rem(g, RING) * ITEMS + j
        src, lanes = pl.ds(start, CHUNK), pl.ds(128 * (j % 2), 128)
        return (pltpu.make_async_copy(k_hbm.at[row, 0, src, :], k_buf.at[slot, :, lanes], k_sem.at[sem]),
                pltpu.make_async_copy(v_hbm.at[row, 0, src, :], v_buf.at[slot, :, lanes], v_sem.at[sem]))

    def launch(g, state):
        b, c = state
        for j in range(ITEMS):
            n = g * ITEMS + j
            item_row[n] = b
            item_chunk[n] = c
            turn = (c + 1 >= chunks_of(b)) & (b < rows - 1)
            b, c = jnp.where(turn, b + 1, b), jnp.where(turn, 0, c + 1)

        @pl.when(g < bodies)
        def _():
            for j in range(ITEMS):
                for copy in copies(g, j):
                    copy.start()
        return b, c

    state = (jnp.int32(0), jnp.int32(0))
    for g in range(RING - 1):
        state = launch(g, state)

    half = BLOCK // 2
    ahead = []
    for p in range(AHEAD):
        columns = pl.ds((EARLY + p) * half, half)
        ahead.append(pltpu.make_async_copy(gate_hbm.at[:, columns], ahead_ref.at[p, :, pl.ds(0, half)], a_sem.at[p, 0]))
        ahead.append(pltpu.make_async_copy(up_hbm.at[:, columns], ahead_ref.at[p, :, pl.ds(half, half)], a_sem.at[p, 1]))
    piece_rows = gate_hbm.shape[0] * AHEAD // PIECES

    def piece(i):
        @pl.when(i < PIECES)
        def _():
            p = lax.div(i, PIECES // AHEAD)
            at = pl.ds(pl.multiple_of(lax.rem(i, PIECES // AHEAD) * piece_rows, piece_rows), piece_rows)
            columns = pl.ds(pl.multiple_of((EARLY + p) * half, half), half)
            pltpu.make_async_copy(gate_hbm.at[at, columns], ahead_ref.at[p, at, pl.ds(0, half)], a_sem.at[p, 0]).start()
            pltpu.make_async_copy(up_hbm.at[at, columns], ahead_ref.at[p, at, pl.ds(half, half)], a_sem.at[p, 1]).start()

    outputs = [pltpu.make_async_copy(k16, key_out, out_sem.at[0]), pltpu.make_async_copy(v16, value_out, out_sem.at[1])]
    for copy in outputs:
        copy.start()
    k_scr[...] = k16[...].astype(F32)
    v_scr[...] = v16[...].astype(F32)
    q_scr[...] = jnp.swapaxes(q_in[...].astype(F32), 0, 1).astype(BF16)
    m_run[...] = jnp.zeros_like(m_run)
    l_run[...] = jnp.ones_like(l_run)
    acc_run[...] = jnp.zeros_like(acc_run)

    def score(g):
        side = lax.rem(g, 2)
        blank = jnp.zeros((head_count, 128), BF16)
        for p in range(ITEMS // 2):
            slot = lax.rem(g, RING) * (ITEMS // 2) + p
            q_rows, lefts = [], []
            for j in range(2):
                n = g * ITEMS + 2 * p + j
                b, c = item_row[n], item_chunk[n]
                q16 = q_scr[b]
                q_rows.append(jnp.concatenate([q16, blank] if j == 0 else [blank, q16], axis=1))
                new_scr[side, 2 * p + j] = jnp.sum(q16.astype(F32) * k_scr[pl.ds(b, 1), :], axis=-1, keepdims=True) * scale
                lefts.append(lengths_ref[base + b] - c * CHUNK)
            s_pair = lax.dot_general(jnp.concatenate(q_rows, axis=0), k_buf[slot], (((1,), (1,)), ((), ())), preferred_element_type=F32) * scale
            for j in range(2):
                s = s_pair[j * head_count:(j + 1) * head_count]
                s = jnp.where(lax.broadcasted_iota(jnp.int32, s.shape, 1) < lefts[j], s, MASK_VALUE)
                s_scr[side, 2 * p + j] = s
                top_scr[side, 2 * p + j] = jnp.max(s, axis=-1, keepdims=True)

    def mix(g):
        side = lax.rem(g, 2)
        m, l, acc = m_run[...], l_run[...], acc_run[...]
        for p in range(ITEMS // 2):
            slot = lax.rem(g, RING) * (ITEMS // 2) + p
            weights, states = [], []
            for j in range(2):
                n = g * ITEMS + 2 * p + j
                b, c = item_row[n], item_chunk[n]
                m_prev = jnp.where(c == 0, new_scr[side, 2 * p + j], m)
                m = jnp.maximum(m_prev, top_scr[side, 2 * p + j])
                e = jnp.exp(s_scr[side, 2 * p + j] - m)
                shrink = jnp.exp(m_prev - m)
                l = jnp.where(c == 0, 1.0, l) * shrink + jnp.sum(e, axis=-1, keepdims=True)
                states.append((b, c, l, shrink))
                weights.append(e.astype(BF16))
            mixed = jnp.dot(jnp.concatenate(weights, axis=0), v_buf[slot], preferred_element_type=F32)
            for j, (b, c, l_item, shrink) in enumerate(states):
                part = mixed[j * head_count:(j + 1) * head_count, j * 128:(j + 1) * 128]
                acc = jnp.where(c == 0, v_scr[pl.ds(b, 1), :], acc) * shrink + part
                o_scr[b] = acc / l_item
        m_run[...], l_run[...], acc_run[...] = m, l, acc

    for j in range(ITEMS):
        copies(0, j)[0].wait()
    score(0)

    def body(g, state):
        state = launch(g + RING - 1, state)
        for k in range(PIECE_STEP):
            piece(g * PIECE_STEP + k)

        @pl.when(g + 1 < bodies)
        def _():
            for j in range(ITEMS):
                copies(g + 1, j)[0].wait()
        for j in range(ITEMS):
            copies(g, j)[1].wait()
        mix(g)
        score(g + 1)
        return state

    lax.fori_loop(0, bodies, body, state)

    def rest(i, _):
        piece(i)
        return 0
    lax.fori_loop(bodies * PIECE_STEP, PIECES, rest, 0)
    for copy in ahead:
        copy.wait()
    for copy in outputs:
        copy.wait()
    o_ref[...] = jnp.swapaxes(o_scr[...], 0, 1).astype(BF16)


def combine_kernel(o_ref, x_hbm, normed, early_ref, ahead_ref, gate_hbm, up_hbm, wo_hbm, wd_hbm, y_ref,
                   act, ring, o_full, x_rows, part, pair_in, in1x, in1y, in2x, in2y,
                   x_sem, sems, o_send, o_recv, c_send, c_recv):
    me = lax.axis_index("model")
    core = lax.rem(me, 2)
    xi = lax.rem(lax.div(me, 2), 2)
    yi = lax.div(me, 4)
    partner = me + 1 - 2 * core
    x_peer = me + 2 - 4 * xi
    y_peer = me + 4 - 8 * yi
    batch = normed.shape[0]
    rows = batch // PEERS
    late = gate_hbm.shape[1] // (BLOCK // 2) - EARLY - AHEAD
    n_chunks = y_ref.shape[1] // CHUNK_COLS
    o_width = wo_hbm.shape[0]
    f_width = wd_hbm.shape[0]
    half = BLOCK // 2
    barrier = greet(me)

    early_width = EARLY * half

    def gu(n, slot):
        return gate_up_copies(n + EARLY + AHEAD, slot, gate_hbm, up_hbm, ring, sems)

    def down(t, slot):
        columns = pl.ds(pl.multiple_of(t * CHUNK_COLS, CHUNK_COLS), CHUNK_COLS)
        lanes = pl.ds(0, CHUNK_COLS)
        return (
            pltpu.make_async_copy(wo_hbm.at[:, columns], ring.at[slot, pl.ds(0, o_width), lanes], sems.at[slot, 0]),
            pltpu.make_async_copy(wd_hbm.at[:, columns], ring.at[slot, pl.ds(o_width, f_width), lanes], sems.at[slot, 1]),
        )

    def fetch(n):
        slot = lax.rem(n, C_SLOTS)

        @pl.when(n < late)
        def _():
            for copy in gu(n, slot):
                copy.start()

        @pl.when((n >= late) & (n < late + n_chunks))
        def _():
            for copy in down(n - late, slot):
                copy.start()

    for copy in gu(0, 0) + gu(1, 1):
        copy.start()
    row_x = core * 128 + xi * 32 + yi * 16
    row_y = core * 128 + 64 + yi * 32 + xi * 16
    x_copies = []
    for k, row in enumerate((row_x, row_y)):
        x_copies.append(pltpu.make_async_copy(x_hbm.at[pl.ds(pl.multiple_of(row, 16), 16), :], x_rows.at[k], x_sem.at[k]))
    pl.semaphore_wait(barrier, PEERS - 1)
    mine = pl.ds(pl.multiple_of(me * rows, rows), rows)
    sends = []
    for step in range(1, PEERS):
        peer = lax.rem(me + step, PEERS)
        sends.append(pltpu.make_async_remote_copy(
            src_ref=o_ref.at[pl.ds(peer * 6, 6)], dst_ref=o_full.at[:, mine, :],
            send_sem=o_send.at[step], recv_sem=o_recv.at[step],
            device_id={"model": peer}, device_id_type=MESH))
        sends[-1].start()
    o_full[:, mine, :] = o_ref[pl.ds(me * 6, 6)]
    act[:, o_width:o_width + early_width] = early_ref[...]
    for p in range(AHEAD):
        at = o_width + early_width + p * half
        act[:, at:at + half] = hidden_block(normed[...], ahead_ref[p])
        if p == 0:
            for copy in gu(2, 2):
                copy.start()
    early_width += AHEAD * half

    def block_step(n, _):
        slot = lax.rem(n, C_SLOTS)
        for copy in gu(n, slot):
            copy.wait()
        at = pl.ds(pl.multiple_of(o_width + early_width + n * half, half), half)
        act[:, at] = hidden_block(normed[...], ring[slot])
        fetch(n + C_SLOTS)
        return 0

    lax.fori_loop(0, late - 1, block_step, 0)
    for copy in x_copies:
        copy.start()
    block_step(late - 1, 0)
    for copy in x_copies:
        copy.wait()
    for copy in sends:
        copy.wait()
    for h in range(6):
        act[:, h * 128:(h + 1) * 128] = o_full[h]

    my_half = pl.multiple_of(core * 128, 128)
    other_half = pl.multiple_of(128 - core * 128, 128)
    keep1x = pl.multiple_of(my_half + xi * 32, 32)
    give1x = pl.multiple_of(my_half + 32 - xi * 32, 32)
    keep1y = pl.multiple_of(my_half + 64 + yi * 32, 32)
    give1y = pl.multiple_of(my_half + 96 - yi * 32, 32)
    keep2x = pl.multiple_of(keep1x + yi * 16, 16)
    give2x = pl.multiple_of(keep1x + 16 - yi * 16, 16)
    keep2y = pl.multiple_of(keep1y + xi * 16, 16)
    give2y = pl.multiple_of(keep1y + 16 - xi * 16, 16)

    def cols(t):
        return pl.ds(pl.multiple_of(t * CHUNK_COLS, CHUNK_COLS), CHUNK_COLS)

    def remote(kind, t, src, dst, peer):
        return pltpu.make_async_remote_copy(
            src_ref=src, dst_ref=dst, send_sem=c_send.at[kind, t], recv_sem=c_recv.at[kind, t],
            device_id={"model": peer}, device_id_type=MESH)

    def pair_sum(t):
        return remote(0, t, part.at[t, pl.ds(other_half, 128), :], pair_in.at[t], partner)

    def scatter1(t):
        return (remote(1, t, part.at[t, pl.ds(give1x, 32), :], in1x.at[t], x_peer),
                remote(2, t, part.at[t, pl.ds(give1y, 32), :], in1y.at[t], y_peer))

    def scatter2(t):
        return (remote(3, t, part.at[t, pl.ds(give2x, 16), :], in2x.at[t], y_peer),
                remote(4, t, part.at[t, pl.ds(give2y, 16), :], in2y.at[t], x_peer))

    def spread(kind, t, row, count, peer):
        at = y_ref.at[pl.ds(row, count), cols(t)]
        return remote(kind, t, at, at, peer)

    def gather1(t):
        return spread(5, t, keep2x, 16, y_peer), spread(6, t, keep2y, 16, x_peer)

    def gather2(t):
        return spread(7, t, keep1x, 32, x_peer), spread(8, t, keep1y, 32, y_peer)

    def pair_copy(t):
        return (spread(9, t, my_half, 128, partner),)

    def start(copies):
        for copy in copies:
            copy.start()

    def arrive(copies):
        for copy in copies:
            copy.wait_recv()

    def stage_compute(t):
        slot = lax.rem(t + late, C_SLOTS)
        for copy in down(t, slot):
            copy.wait()
        part[t] = jnp.dot(act[...], ring[slot, pl.ds(0, o_width + f_width), pl.ds(0, CHUNK_COLS)], preferred_element_type=F32)
        pair_sum(t).start()
        fetch(t + late + C_SLOTS)

    def stage_scatter1(t):
        pair_sum(t).wait_recv()
        part[t, pl.ds(my_half, 128), :] = part[t, pl.ds(my_half, 128), :] + pair_in[t]
        start(scatter1(t))

    def stage_scatter2(t):
        arrive(scatter1(t))
        part[t, pl.ds(keep1x, 32), :] = part[t, pl.ds(keep1x, 32), :] + in1x[t]
        part[t, pl.ds(keep1y, 32), :] = part[t, pl.ds(keep1y, 32), :] + in1y[t]
        start(scatter2(t))

    def stage_gather1(t):
        arrive(scatter2(t))
        for k, (keep, inbox) in enumerate(((keep2x, in2x), (keep2y, in2y))):
            total = part[t, pl.ds(keep, 16), :] + inbox[t]
            y_ref[pl.ds(keep, 16), cols(t)] = (x_rows[k, :, cols(t)].astype(F32) + total).astype(BF16)
        start(gather1(t))

    def stage_gather2(t):
        arrive(gather1(t))
        start(gather2(t))

    def stage_pair(t):
        arrive(gather2(t))
        start(pair_copy(t))

    def stage_end(t):
        arrive(pair_copy(t))

    stages = (stage_compute, stage_scatter1, stage_scatter2, stage_gather1, stage_gather2, stage_pair, stage_end)

    def iteration(i, _):
        for lag, stage in zip(LAGS, stages):
            t = i - lag

            @pl.when((t >= 0) & (t < n_chunks))
            def _(stage=stage, t=t):
                stage(t)
        return 0

    lax.fori_loop(0, n_chunks + LAGS[-1], iteration, 0)

    def drain(t, _):
        for copy in (pair_sum(t),) + scatter1(t) + scatter2(t) + gather1(t) + gather2(t) + pair_copy(t):
            copy.wait_send()
        return 0

    lax.fori_loop(0, n_chunks, drain, 0)


ANY = pl.BlockSpec(memory_space=pltpu.HBM)
VM = pl.BlockSpec(memory_space=pltpu.VMEM)
SM = pl.BlockSpec(memory_space=pltpu.SMEM)
LIMIT = 50 << 20


def project_call(tokens, lengths, norm_gain, w_query, w_key, w_value, w_gate, w_up):
    lengths, norm_gain = (pltpu.with_memory_space_constraint(a, pltpu.HBM) for a in (lengths, norm_gain))
    batch, width = tokens.shape
    rows = batch // PEERS
    dma = pltpu.SemaphoreType.DMA
    return pl.pallas_call(
        project_kernel,
        name="project",
        out_shape=(
            pltpu.VMEM((width // 128, rows, 128), BF16),
            pltpu.VMEM((rows, 128), BF16),
            pltpu.VMEM((rows, 128), BF16),
            pltpu.VMEM((batch, width), BF16),
            pltpu.VMEM((batch, EARLY * BLOCK // 2), BF16),
        ),
        in_specs=[ANY, ANY, ANY, ANY, ANY, ANY, ANY, ANY],
        out_specs=(VM, VM, VM, VM, VM),
        scratch_shapes=[
            pltpu.VMEM((batch, width), BF16),
            pltpu.VMEM((batch,), jnp.int32),
            pltpu.VMEM((width,), BF16),
            pltpu.VMEM((SLOTS, width, BLOCK), BF16),
            pltpu.VMEM((6, batch, 128), BF16),
            pltpu.VMEM((batch, 128), F32),
            pltpu.VMEM((batch, 128), F32),
            pltpu.VMEM((batch, 128), F32),
            pltpu.VMEM((1, width), F32),
            dma, dma((2,)), dma((SLOTS, 3)), dma((PEERS,)), dma((PEERS,)),
        ],
        compiler_params=pltpu.CompilerParams(collective_id=0, has_side_effects=True, vmem_limit_bytes=LIMIT),
    )(tokens, lengths, norm_gain, w_query, w_key, w_value, w_gate, w_up)


def attend_call(lengths, q_all, key_new, value_new, k_cache, v_cache, w_gate, w_up):
    heads, rows, _ = q_all.shape
    dma = pltpu.SemaphoreType.DMA
    return pl.pallas_call(
        attend_kernel,
        name="attend",
        out_shape=(
            pltpu.VMEM((heads, rows, 128), BF16),
            jax.ShapeDtypeStruct((rows, 128), BF16),
            jax.ShapeDtypeStruct((rows, 128), BF16),
            pltpu.VMEM((AHEAD, w_gate.shape[0], BLOCK), BF16),
        ),
        in_specs=[SM, VM, VM, VM, ANY, ANY, ANY, ANY],
        out_specs=(VM, ANY, ANY, VM),
        scratch_shapes=[
            pltpu.VMEM((rows, heads, 128), BF16),
            pltpu.VMEM((rows, heads, 128), F32),
            pltpu.VMEM((rows, 128), F32),
            pltpu.VMEM((rows, 128), F32),
            pltpu.VMEM((2, ITEMS, heads, CHUNK), F32),
            pltpu.VMEM((2, ITEMS, heads, 1), F32),
            pltpu.VMEM((2, ITEMS, heads, 1), F32),
            pltpu.VMEM((RING * ITEMS // 2, CHUNK, 256), BF16),
            pltpu.VMEM((RING * ITEMS // 2, CHUNK, 256), BF16),
            pltpu.SMEM((rows * (k_cache.shape[2] // CHUNK) + RING * ITEMS,), jnp.int32),
            pltpu.SMEM((rows * (k_cache.shape[2] // CHUNK) + RING * ITEMS,), jnp.int32),
            pltpu.VMEM((heads, 1), F32),
            pltpu.VMEM((heads, 1), F32),
            pltpu.VMEM((heads, 128), F32),
            dma((RING * ITEMS,)), dma((RING * ITEMS,)), dma((2,)), dma((AHEAD, 2)),
        ],
        compiler_params=pltpu.CompilerParams(vmem_limit_bytes=20 << 20),
    )(lengths, q_all, key_new, value_new, k_cache, v_cache, w_gate, w_up)


def combine_call(attended, tokens, normed, early, ahead, w_gate, w_up, w_out, w_down):
    attended, normed, early, ahead = (pltpu.with_memory_space_constraint(a, pltpu.VMEM) for a in (attended, normed, early, ahead))
    batch, width = tokens.shape
    n_chunks = width // CHUNK_COLS
    dma = pltpu.SemaphoreType.DMA
    return pl.pallas_call(
        combine_kernel,
        name="combine",
        out_shape=pltpu.VMEM((batch, width), BF16),
        in_specs=[VM, ANY, VM, VM, VM, ANY, ANY, ANY, ANY],
        out_specs=VM,
        scratch_shapes=[
            pltpu.VMEM((batch, w_out.shape[0] + w_down.shape[0]), BF16),
            pltpu.VMEM((C_SLOTS, width, BLOCK), BF16),
            pltpu.VMEM((6, batch, 128), BF16),
            pltpu.VMEM((2, 16, width), BF16),
            pltpu.VMEM((n_chunks, batch, CHUNK_COLS), F32),
            pltpu.VMEM((n_chunks, 128, CHUNK_COLS), F32),
            pltpu.VMEM((n_chunks, 32, CHUNK_COLS), F32),
            pltpu.VMEM((n_chunks, 32, CHUNK_COLS), F32),
            pltpu.VMEM((n_chunks, 16, CHUNK_COLS), F32),
            pltpu.VMEM((n_chunks, 16, CHUNK_COLS), F32),
            dma((2,)), dma((C_SLOTS, 2)), dma((PEERS,)), dma((PEERS,)),
            dma((10, n_chunks)), dma((10, n_chunks)),
        ],
        compiler_params=pltpu.CompilerParams(collective_id=1, has_side_effects=True, vmem_limit_bytes=40 << 20),
    )(attended, tokens, normed, early, ahead, w_gate, w_up, w_out, w_down)


def solution(mesh):
    def local_step(tokens, lengths, k_cache, v_cache, norm_gain, w_query, w_key, w_value, w_out, w_gate, w_up, w_down):
        rows = tokens.shape[0] // PEERS
        q_all, key_new, value_new, normed, early = project_call(tokens, lengths, norm_gain, w_query, w_key, w_value, w_gate, w_up)
        attended, key_new, value_new, ahead = attend_call(lengths, q_all, key_new, value_new, k_cache, v_cache, w_gate, w_up)
        y = combine_call(attended, tokens, normed, early, ahead, w_gate, w_up, w_out, w_down)
        return y, key_new.reshape(rows, 1, 128), value_new.reshape(rows, 1, 128)

    in_specs = (P('replica', None), P('replica'), P('replica', None, None, None), P('replica', None, None, None), P(None), P(None, 'model'), P(None, None), P(None, None), P('model', None), P(None, 'model'), P(None, 'model'), P('model', None))
    out_specs = (P('replica', None), P(('replica', 'model'), None, None), P(('replica', 'model'), None, None))
    return jax.shard_map(local_step, mesh=mesh, in_specs=in_specs, out_specs=out_specs, check_vma=False)
```

```python
import functools
import math
import jax
import jax.numpy as jnp
from jax import lax
from jax.experimental import pallas as pl
from jax.experimental.pallas import tpu as pltpu
from jax.sharding import PartitionSpec as P

ROPE_BASE = 10000.0
NORM_EPS = 1e-6
MASK_VALUE = -1e30
BF16, F32 = jnp.bfloat16, jnp.float32
MESH = pl.DeviceIdType.MESH

PEERS = 8
SLOTS = 4
BLOCK = 512
EARLY = 4
CHUNK = 512
ITEMS = 8
PIECES = 12
PIECE_STEP = 2
AHEAD = 2
C_SLOTS = 3
RING = 5
CHUNK_COLS = 512
LAGS = (0, 1, 4, 10, 14, 18, 19)


def greet(me):
    barrier = pltpu.get_barrier_semaphore()
    for step in range(1, PEERS):
        peer = lax.rem(me + step, PEERS)
        pl.semaphore_signal(barrier, inc=1, device_id={"model": peer}, device_id_type=MESH)
    return barrier


def gate_up_copies(block, slot, gate_hbm, up_hbm, ring, sems):
    half = BLOCK // 2
    columns = pl.ds(pl.multiple_of(block * half, half), half)
    return (
        pltpu.make_async_copy(gate_hbm.at[:, columns], ring.at[slot, :, pl.ds(0, half)], sems.at[slot, 0]),
        pltpu.make_async_copy(up_hbm.at[:, columns], ring.at[slot, :, pl.ds(half, half)], sems.at[slot, 1]),
    )


def hidden_block(normed, weights):
    half = BLOCK // 2
    both = jnp.dot(normed, weights, preferred_element_type=F32)
    gate, up = both[:, :half], both[:, half:]
    return (gate * lax.logistic(gate) * up).astype(BF16)


def rope(values, cos_part, sin_part):
    return values * cos_part + pltpu.roll(values, 64, 1) * sin_part


def project_kernel(x_hbm, lengths_hbm, gain_hbm, wq_hbm, wk_hbm, wv_hbm, gate_hbm, up_hbm,
                   q_out, knew_ref, vnew_ref, normed, hidden_ref,
                   x_ref, lengths_ref, gain_ref, ring, q_scr, cos_scr, sin_scr, stat_scr, gain_scr, x_sem, in_sem, sems, send_sem, recv_sem):
    me = lax.axis_index("model")
    batch = x_ref.shape[0]
    width = x_ref.shape[1]
    rows = batch // PEERS
    barrier = greet(me)
    x_copy = pltpu.make_async_copy(x_hbm, x_ref, x_sem)
    l_copy = pltpu.make_async_copy(lengths_hbm, lengths_ref, in_sem.at[0])
    g_copy = pltpu.make_async_copy(gain_hbm, gain_ref, in_sem.at[1])
    for copy in (l_copy, x_copy, g_copy):
        copy.start()
    first = (pltpu.make_async_copy(wq_hbm.at[:, pl.ds(0, 512)], ring.at[0], sems.at[0, 0]),)
    second = (
        pltpu.make_async_copy(wq_hbm.at[:, pl.ds(512, 256)], ring.at[1, :, pl.ds(0, 256)], sems.at[1, 0]),
        pltpu.make_async_copy(wk_hbm, ring.at[1, :, pl.ds(256, 128)], sems.at[1, 1]),
        pltpu.make_async_copy(wv_hbm, ring.at[1, :, pl.ds(384, 128)], sems.at[1, 2]),
    )
    gu = lambda block, slot: gate_up_copies(block, slot, gate_hbm, up_hbm, ring, sems)

    for copy in first:
        copy.start()

    hb = batch // 2
    l_copy.wait()
    spread = jnp.broadcast_to(lengths_ref[...].astype(F32).reshape(1, batch), (128, batch)).T
    lane = lax.broadcasted_iota(jnp.int32, (hb, 128), 1)
    low = lane < 64
    pair = jnp.where(low, lane, lane - 64).astype(F32)
    inv_freq = jnp.exp(pair * (-2.0 * math.log(ROPE_BASE) / 128))
    angles = jnp.where(low, spread[:hb], spread[hb:]) * inv_freq
    cos_part, sin_part = jnp.cos(angles), jnp.sin(angles)
    cos_turn, sin_turn = pltpu.roll(cos_part, 64, 1), pltpu.roll(sin_part, 64, 1)
    cos_scr[:hb] = jnp.where(low, cos_part, cos_turn)
    cos_scr[hb:] = jnp.where(low, cos_turn, cos_part)
    sin_scr[:hb] = jnp.where(low, -sin_part, sin_turn)
    sin_scr[hb:] = jnp.where(low, -sin_turn, sin_part)

    x_copy.wait()
    tiles = width // 128

    def square_rows(r, _):
        at = pl.ds(pl.multiple_of(r * 16, 16), 16)
        sums = [jnp.zeros((16, 128), F32) for _ in range(4)]
        for j in range(tiles):
            values = x_ref[at, j * 128:(j + 1) * 128].astype(F32)
            sums[j % 4] = sums[j % 4] + values * values
        stat_scr[at, :] = (sums[0] + sums[1]) + (sums[2] + sums[3])
        return 0

    lax.fori_loop(0, batch // 16, square_rows, 0)
    mean_sq = jnp.sum(stat_scr[...], axis=-1, keepdims=True) * (1.0 / width)
    stat_scr[...] = jnp.broadcast_to(lax.rsqrt(mean_sq + NORM_EPS), (batch, 128))

    def norm_rows(r, _):
        at = pl.ds(pl.multiple_of(r * 16, 16), 16)
        factor = stat_scr[at, :]
        for j in range(tiles):
            cols = slice(j * 128, (j + 1) * 128)
            normed[at, cols] = (x_ref[at, cols].astype(F32) * factor * gain_scr[:, cols]).astype(BF16)
        return 0

    for copy in second:
        copy.start()
    g_copy.wait()
    gain_scr[...] = gain_ref[...].astype(F32).reshape(1, width)
    lax.fori_loop(0, batch // 16, norm_rows, 0)

    for copy in first:
        copy.wait()
    for copy in gu(0, 2):
        copy.start()
    head4 = jnp.dot(normed[...], ring[0], preferred_element_type=F32)
    for h in range(4):
        q_scr[h] = rope(head4[:, h * 128:(h + 1) * 128], cos_scr[...], sin_scr[...]).astype(BF16)
    for copy in second:
        copy.wait()
    for copy in gu(1, 3) + gu(2, 0):
        copy.start()
    tail = jnp.dot(normed[...], ring[1], preferred_element_type=F32)
    for h in range(2):
        q_scr[4 + h] = rope(tail[:, h * 128:(h + 1) * 128], cos_scr[...], sin_scr[...]).astype(BF16)
    k_all = rope(tail[:, 256:384], cos_scr[...], sin_scr[...])
    cos_scr[...] = k_all
    sin_scr[...] = tail[:, 384:512]
    mine = pl.ds(pl.multiple_of(me * rows, rows), rows)
    knew_ref[...] = cos_scr[mine, :].astype(BF16)
    vnew_ref[...] = sin_scr[mine, :].astype(BF16)
    for copy in gu(3, 1):
        copy.start()

    pl.semaphore_wait(barrier, PEERS - 1)
    heads = pl.ds(me * 6, 6)
    sends = []
    for step in range(1, PEERS):
        peer = lax.rem(me + step, PEERS)
        sends.append(pltpu.make_async_remote_copy(
            src_ref=q_scr.at[:, pl.ds(pl.multiple_of(peer * rows, rows), rows), :],
            dst_ref=q_out.at[heads],
            send_sem=send_sem.at[step], recv_sem=recv_sem.at[step],
            device_id={"model": peer}, device_id_type=MESH))
        sends[-1].start()
    q_out[heads] = q_scr[:, mine, :]

    half = BLOCK // 2

    def block_step(n, _):
        slot = lax.rem(n + 2, SLOTS)
        for copy in gu(n, slot):
            copy.wait()
        hidden_ref[:, pl.ds(pl.multiple_of(n * half, half), half)] = hidden_block(normed[...], ring[slot])

        @pl.when(n + SLOTS < EARLY)
        def _():
            for copy in gu(n + SLOTS, slot):
                copy.start()
        return 0

    lax.fori_loop(0, EARLY, block_step, 0)
    for copy in sends:
        copy.wait()


def attend_kernel(lengths_ref, q_in, k16, v16, k_hbm, v_hbm, gate_hbm, up_hbm, o_ref, key_out, value_out, ahead_ref,
                  q_scr, o_scr, k_scr, v_scr, s_scr, top_scr, new_scr, k_buf, v_buf, item_row, item_chunk, m_run, l_run, acc_run,
                  k_sem, v_sem, out_sem, a_sem):
    me = lax.axis_index("model")
    rows = o_ref.shape[1]
    head_count = o_ref.shape[0]
    context = k_hbm.shape[2]
    base = me * rows
    scale = 128 ** -0.5
    def chunks_of(b):
        return lax.div(lengths_ref[base + b] + (CHUNK - 1), CHUNK)

    total = chunks_of(0)
    for b in range(1, rows):
        total = total + chunks_of(b)
    bodies = lax.div(total + (ITEMS - 1), ITEMS)

    def copies(g, j):
        n = g * ITEMS + j
        start = pl.multiple_of(jnp.minimum(item_chunk[n] * CHUNK, context - CHUNK), CHUNK)
        row = base + item_row[n]
        slot = lax.rem(g, RING) * (ITEMS // 2) + j // 2
        sem = lax.rem(g, RING)
        src, lanes = pl.ds(start, CHUNK), pl.ds(128 * (j % 2), 128)
        return (pltpu.make_async_copy(k_hbm.at[row, 0, src, :], k_buf.at[slot, :, lanes], k_sem.at[sem]),
                pltpu.make_async_copy(v_hbm.at[row, 0, src, :], v_buf.at[slot, :, lanes], v_sem.at[sem]))

    def arrived(g, buf, sems):
        at = buf.at[pl.ds(lax.rem(g, RING) * (ITEMS // 2), ITEMS // 2)]
        pltpu.make_async_copy(at, at, sems.at[lax.rem(g, RING)]).wait()

    def launch(g, state):
        b, c = state
        for j in range(ITEMS):
            n = g * ITEMS + j
            item_row[n] = b
            item_chunk[n] = c
            turn = (c + 1 >= chunks_of(b)) & (b < rows - 1)
            b, c = jnp.where(turn, b + 1, b), jnp.where(turn, 0, c + 1)

        @pl.when(g < bodies)
        def _():
            for j in range(ITEMS):
                for copy in copies(g, j):
                    copy.start()
        return b, c

    state = (jnp.int32(0), jnp.int32(0))
    for g in range(RING - 1):
        state = launch(g, state)

    half = BLOCK // 2
    ahead = []
    for p in range(AHEAD):
        columns = pl.ds((EARLY + p) * half, half)
        ahead.append(pltpu.make_async_copy(gate_hbm.at[:, columns], ahead_ref.at[p, :, pl.ds(0, half)], a_sem.at[p, 0]))
        ahead.append(pltpu.make_async_copy(up_hbm.at[:, columns], ahead_ref.at[p, :, pl.ds(half, half)], a_sem.at[p, 1]))
    piece_rows = gate_hbm.shape[0] * AHEAD // PIECES

    def piece(i):
        @pl.when(i < PIECES)
        def _():
            p = lax.div(i, PIECES // AHEAD)
            at = pl.ds(pl.multiple_of(lax.rem(i, PIECES // AHEAD) * piece_rows, piece_rows), piece_rows)
            columns = pl.ds(pl.multiple_of((EARLY + p) * half, half), half)
            pltpu.make_async_copy(gate_hbm.at[at, columns], ahead_ref.at[p, at, pl.ds(0, half)], a_sem.at[p, 0]).start()
            pltpu.make_async_copy(up_hbm.at[at, columns], ahead_ref.at[p, at, pl.ds(half, half)], a_sem.at[p, 1]).start()

    outputs = [pltpu.make_async_copy(k16, key_out, out_sem.at[0]), pltpu.make_async_copy(v16, value_out, out_sem.at[1])]
    for copy in outputs:
        copy.start()
    k_scr[...] = k16[...].astype(F32)
    v_scr[...] = v16[...].astype(F32)
    q_scr[...] = jnp.swapaxes(q_in[...].astype(F32), 0, 1).astype(BF16)
    m_run[...] = jnp.zeros_like(m_run)
    l_run[...] = jnp.ones_like(l_run)
    acc_run[...] = jnp.zeros_like(acc_run)

    def score(g):
        side = lax.rem(g, 2)
        blank = jnp.zeros((head_count, 128), BF16)
        for p in range(ITEMS // 2):
            slot = lax.rem(g, RING) * (ITEMS // 2) + p
            q_rows, lefts = [], []
            for j in range(2):
                n = g * ITEMS + 2 * p + j
                b, c = item_row[n], item_chunk[n]
                q16 = q_scr[b]
                q_rows.append(jnp.concatenate([q16, blank] if j == 0 else [blank, q16], axis=1))
                new_scr[side, 2 * p + j] = jnp.sum(q16.astype(F32) * k_scr[pl.ds(b, 1), :], axis=-1, keepdims=True) * scale
                lefts.append(lengths_ref[base + b] - c * CHUNK)
            s_pair = lax.dot_general(jnp.concatenate(q_rows, axis=0), k_buf[slot], (((1,), (1,)), ((), ())), preferred_element_type=F32) * scale
            for j in range(2):
                s = s_pair[j * head_count:(j + 1) * head_count]
                s = jnp.where(lax.broadcasted_iota(jnp.int32, s.shape, 1) < lefts[j], s, MASK_VALUE)
                s_scr[side, 2 * p + j] = s
                top_scr[side, 2 * p + j] = jnp.max(s, axis=-1, keepdims=True)

    def mix(g):
        side = lax.rem(g, 2)
        m, l, acc = m_run[...], l_run[...], acc_run[...]
        for p in range(ITEMS // 2):
            slot = lax.rem(g, RING) * (ITEMS // 2) + p
            weights, states = [], []
            for j in range(2):
                n = g * ITEMS + 2 * p + j
                b, c = item_row[n], item_chunk[n]
                m_prev = jnp.where(c == 0, new_scr[side, 2 * p + j], m)
                m = jnp.maximum(m_prev, top_scr[side, 2 * p + j])
                e = jnp.exp(s_scr[side, 2 * p + j] - m)
                shrink = jnp.exp(m_prev - m)
                l = jnp.where(c == 0, 1.0, l) * shrink + jnp.sum(e, axis=-1, keepdims=True)
                states.append((b, c, l, shrink))
                weights.append(e.astype(BF16))
            mixed = jnp.dot(jnp.concatenate(weights, axis=0), v_buf[slot], preferred_element_type=F32)
            for j, (b, c, l_item, shrink) in enumerate(states):
                part = mixed[j * head_count:(j + 1) * head_count, j * 128:(j + 1) * 128]
                acc = jnp.where(c == 0, v_scr[pl.ds(b, 1), :], acc) * shrink + part
                o_scr[b] = acc / l_item
        m_run[...], l_run[...], acc_run[...] = m, l, acc

    arrived(0, k_buf, k_sem)
    score(0)

    def body(g, state):
        state = launch(g + RING - 1, state)
        for k in range(PIECE_STEP):
            piece(g * PIECE_STEP + k)

        @pl.when(g + 1 < bodies)
        def _():
            arrived(g + 1, k_buf, k_sem)
        arrived(g, v_buf, v_sem)
        mix(g)
        score(g + 1)
        return state

    lax.fori_loop(0, bodies, body, state)

    def rest(i, _):
        piece(i)
        return 0
    lax.fori_loop(bodies * PIECE_STEP, PIECES, rest, 0)
    for copy in ahead:
        copy.wait()
    for copy in outputs:
        copy.wait()
    o_ref[...] = jnp.swapaxes(o_scr[...], 0, 1).astype(BF16)


def combine_kernel(o_ref, x_hbm, normed, early_ref, ahead_ref, gate_hbm, up_hbm, wo_hbm, wd_hbm, y_ref,
                   act, ring, o_full, x_rows, part, pair_in, in1x, in1y, in2x, in2y,
                   x_sem, sems, o_send, o_recv, c_send, c_recv):
    me = lax.axis_index("model")
    core = lax.rem(me, 2)
    xi = lax.rem(lax.div(me, 2), 2)
    yi = lax.div(me, 4)
    partner = me + 1 - 2 * core
    x_peer = me + 2 - 4 * xi
    y_peer = me + 4 - 8 * yi
    batch = normed.shape[0]
    rows = batch // PEERS
    late = gate_hbm.shape[1] // (BLOCK // 2) - EARLY - AHEAD
    n_chunks = y_ref.shape[1] // CHUNK_COLS
    o_width = wo_hbm.shape[0]
    f_width = wd_hbm.shape[0]
    half = BLOCK // 2
    barrier = greet(me)

    early_width = EARLY * half

    def gu(n, slot):
        return gate_up_copies(n + EARLY + AHEAD, slot, gate_hbm, up_hbm, ring, sems)

    def down(t, slot):
        columns = pl.ds(pl.multiple_of(t * CHUNK_COLS, CHUNK_COLS), CHUNK_COLS)
        lanes = pl.ds(0, CHUNK_COLS)
        return (
            pltpu.make_async_copy(wo_hbm.at[:, columns], ring.at[slot, pl.ds(0, o_width), lanes], sems.at[slot, 0]),
            pltpu.make_async_copy(wd_hbm.at[:, columns], ring.at[slot, pl.ds(o_width, f_width), lanes], sems.at[slot, 1]),
        )

    def fetch(n):
        slot = lax.rem(n, C_SLOTS)

        @pl.when(n < late)
        def _():
            for copy in gu(n, slot):
                copy.start()

        @pl.when((n >= late) & (n < late + n_chunks))
        def _():
            for copy in down(n - late, slot):
                copy.start()

    for copy in gu(0, 0) + gu(1, 1):
        copy.start()
    row_x = core * 128 + xi * 32 + yi * 16
    row_y = core * 128 + 64 + yi * 32 + xi * 16
    x_copies = []
    for k, row in enumerate((row_x, row_y)):
        x_copies.append(pltpu.make_async_copy(x_hbm.at[pl.ds(pl.multiple_of(row, 16), 16), :], x_rows.at[k], x_sem.at[k]))
    pl.semaphore_wait(barrier, PEERS - 1)
    mine = pl.ds(pl.multiple_of(me * rows, rows), rows)
    sends = []
    for step in range(1, PEERS):
        peer = lax.rem(me + step, PEERS)
        sends.append(pltpu.make_async_remote_copy(
            src_ref=o_ref.at[pl.ds(peer * 6, 6)], dst_ref=o_full.at[:, mine, :],
            send_sem=o_send.at[step], recv_sem=o_recv.at[step],
            device_id={"model": peer}, device_id_type=MESH))
        sends[-1].start()
    o_full[:, mine, :] = o_ref[pl.ds(me * 6, 6)]
    act[:, o_width:o_width + early_width] = early_ref[...]
    for p in range(AHEAD):
        at = o_width + early_width + p * half
        act[:, at:at + half] = hidden_block(normed[...], ahead_ref[p])
        if p == 0:
            for copy in gu(2, 2):
                copy.start()
    early_width += AHEAD * half

    def block_step(n, _):
        slot = lax.rem(n, C_SLOTS)
        for copy in gu(n, slot):
            copy.wait()
        at = pl.ds(pl.multiple_of(o_width + early_width + n * half, half), half)
        act[:, at] = hidden_block(normed[...], ring[slot])
        fetch(n + C_SLOTS)
        return 0

    lax.fori_loop(0, late - 1, block_step, 0)
    for copy in x_copies:
        copy.start()
    block_step(late - 1, 0)
    for copy in x_copies:
        copy.wait()
    for copy in sends:
        copy.wait()
    for h in range(6):
        act[:, h * 128:(h + 1) * 128] = o_full[h]

    my_half = pl.multiple_of(core * 128, 128)
    other_half = pl.multiple_of(128 - core * 128, 128)
    keep1x = pl.multiple_of(my_half + xi * 32, 32)
    give1x = pl.multiple_of(my_half + 32 - xi * 32, 32)
    keep1y = pl.multiple_of(my_half + 64 + yi * 32, 32)
    give1y = pl.multiple_of(my_half + 96 - yi * 32, 32)
    keep2x = pl.multiple_of(keep1x + yi * 16, 16)
    give2x = pl.multiple_of(keep1x + 16 - yi * 16, 16)
    keep2y = pl.multiple_of(keep1y + xi * 16, 16)
    give2y = pl.multiple_of(keep1y + 16 - xi * 16, 16)

    def cols(t):
        return pl.ds(pl.multiple_of(t * CHUNK_COLS, CHUNK_COLS), CHUNK_COLS)

    def remote(kind, t, src, dst, peer):
        return pltpu.make_async_remote_copy(
            src_ref=src, dst_ref=dst, send_sem=c_send.at[kind, t], recv_sem=c_recv.at[kind, t],
            device_id={"model": peer}, device_id_type=MESH)

    def pair_sum(t):
        return remote(0, t, part.at[t, pl.ds(other_half, 128), :], pair_in.at[t], partner)

    def scatter1(t):
        return (remote(1, t, part.at[t, pl.ds(give1x, 32), :], in1x.at[t], x_peer),
                remote(2, t, part.at[t, pl.ds(give1y, 32), :], in1y.at[t], y_peer))

    def scatter2(t):
        return (remote(3, t, part.at[t, pl.ds(give2x, 16), :], in2x.at[t], y_peer),
                remote(4, t, part.at[t, pl.ds(give2y, 16), :], in2y.at[t], x_peer))

    def spread(kind, t, row, count, peer):
        at = y_ref.at[pl.ds(row, count), cols(t)]
        return remote(kind, t, at, at, peer)

    def gather1(t):
        return spread(5, t, keep2x, 16, y_peer), spread(6, t, keep2y, 16, x_peer)

    def gather2(t):
        return spread(7, t, keep1x, 32, x_peer), spread(8, t, keep1y, 32, y_peer)

    def pair_copy(t):
        return (spread(9, t, my_half, 128, partner),)

    def start(copies):
        for copy in copies:
            copy.start()

    def arrive(copies):
        for copy in copies:
            copy.wait_recv()

    def stage_compute(t):
        slot = lax.rem(t + late, C_SLOTS)
        for copy in down(t, slot):
            copy.wait()
        part[t] = jnp.dot(act[...], ring[slot, pl.ds(0, o_width + f_width), pl.ds(0, CHUNK_COLS)], preferred_element_type=F32)
        pair_sum(t).start()
        fetch(t + late + C_SLOTS)

    def stage_scatter1(t):
        pair_sum(t).wait_recv()
        part[t, pl.ds(my_half, 128), :] = part[t, pl.ds(my_half, 128), :] + pair_in[t]
        start(scatter1(t))

    def stage_scatter2(t):
        arrive(scatter1(t))
        part[t, pl.ds(keep1x, 32), :] = part[t, pl.ds(keep1x, 32), :] + in1x[t]
        part[t, pl.ds(keep1y, 32), :] = part[t, pl.ds(keep1y, 32), :] + in1y[t]
        start(scatter2(t))

    def stage_gather1(t):
        arrive(scatter2(t))
        for k, (keep, inbox) in enumerate(((keep2x, in2x), (keep2y, in2y))):
            total = part[t, pl.ds(keep, 16), :] + inbox[t]
            y_ref[pl.ds(keep, 16), cols(t)] = (x_rows[k, :, cols(t)].astype(F32) + total).astype(BF16)
        start(gather1(t))

    def stage_gather2(t):
        arrive(gather1(t))
        start(gather2(t))

    def stage_pair(t):
        arrive(gather2(t))
        start(pair_copy(t))

    def stage_end(t):
        arrive(pair_copy(t))

    stages = (stage_compute, stage_scatter1, stage_scatter2, stage_gather1, stage_gather2, stage_pair, stage_end)

    def iteration(i, _):
        for lag, stage in zip(LAGS, stages):
            t = i - lag

            @pl.when((t >= 0) & (t < n_chunks))
            def _(stage=stage, t=t):
                stage(t)
        return 0

    lax.fori_loop(0, n_chunks + LAGS[-1], iteration, 0)

    def drain(t, _):
        for copy in (pair_sum(t),) + scatter1(t) + scatter2(t) + gather1(t) + gather2(t) + pair_copy(t):
            copy.wait_send()
        return 0

    lax.fori_loop(0, n_chunks, drain, 0)


ANY = pl.BlockSpec(memory_space=pltpu.HBM)
VM = pl.BlockSpec(memory_space=pltpu.VMEM)
SM = pl.BlockSpec(memory_space=pltpu.SMEM)
LIMIT = 50 << 20


def project_call(tokens, lengths, norm_gain, w_query, w_key, w_value, w_gate, w_up):
    lengths, norm_gain = (pltpu.with_memory_space_constraint(a, pltpu.HBM) for a in (lengths, norm_gain))
    batch, width = tokens.shape
    rows = batch // PEERS
    dma = pltpu.SemaphoreType.DMA
    return pl.pallas_call(
        project_kernel,
        name="project",
        out_shape=(
            pltpu.VMEM((width // 128, rows, 128), BF16),
            pltpu.VMEM((rows, 128), BF16),
            pltpu.VMEM((rows, 128), BF16),
            pltpu.VMEM((batch, width), BF16),
            pltpu.VMEM((batch, EARLY * BLOCK // 2), BF16),
        ),
        in_specs=[ANY, ANY, ANY, ANY, ANY, ANY, ANY, ANY],
        out_specs=(VM, VM, VM, VM, VM),
        scratch_shapes=[
            pltpu.VMEM((batch, width), BF16),
            pltpu.VMEM((batch,), jnp.int32),
            pltpu.VMEM((width,), BF16),
            pltpu.VMEM((SLOTS, width, BLOCK), BF16),
            pltpu.VMEM((6, batch, 128), BF16),
            pltpu.VMEM((batch, 128), F32),
            pltpu.VMEM((batch, 128), F32),
            pltpu.VMEM((batch, 128), F32),
            pltpu.VMEM((1, width), F32),
            dma, dma((2,)), dma((SLOTS, 3)), dma((PEERS,)), dma((PEERS,)),
        ],
        compiler_params=pltpu.CompilerParams(collective_id=0, has_side_effects=True, vmem_limit_bytes=LIMIT),
    )(tokens, lengths, norm_gain, w_query, w_key, w_value, w_gate, w_up)


def attend_call(lengths, q_all, key_new, value_new, k_cache, v_cache, w_gate, w_up):
    heads, rows, _ = q_all.shape
    dma = pltpu.SemaphoreType.DMA
    return pl.pallas_call(
        attend_kernel,
        name="attend",
        out_shape=(
            pltpu.VMEM((heads, rows, 128), BF16),
            jax.ShapeDtypeStruct((rows, 128), BF16),
            jax.ShapeDtypeStruct((rows, 128), BF16),
            pltpu.VMEM((AHEAD, w_gate.shape[0], BLOCK), BF16),
        ),
        in_specs=[SM, VM, VM, VM, ANY, ANY, ANY, ANY],
        out_specs=(VM, ANY, ANY, VM),
        scratch_shapes=[
            pltpu.VMEM((rows, heads, 128), BF16),
            pltpu.VMEM((rows, heads, 128), F32),
            pltpu.VMEM((rows, 128), F32),
            pltpu.VMEM((rows, 128), F32),
            pltpu.VMEM((2, ITEMS, heads, CHUNK), F32),
            pltpu.VMEM((2, ITEMS, heads, 1), F32),
            pltpu.VMEM((2, ITEMS, heads, 1), F32),
            pltpu.VMEM((RING * ITEMS // 2, CHUNK, 256), BF16),
            pltpu.VMEM((RING * ITEMS // 2, CHUNK, 256), BF16),
            pltpu.SMEM((rows * (k_cache.shape[2] // CHUNK) + RING * ITEMS,), jnp.int32),
            pltpu.SMEM((rows * (k_cache.shape[2] // CHUNK) + RING * ITEMS,), jnp.int32),
            pltpu.VMEM((heads, 1), F32),
            pltpu.VMEM((heads, 1), F32),
            pltpu.VMEM((heads, 128), F32),
            dma((RING,)), dma((RING,)), dma((2,)), dma((AHEAD, 2)),
        ],
        compiler_params=pltpu.CompilerParams(vmem_limit_bytes=20 << 20),
    )(lengths, q_all, key_new, value_new, k_cache, v_cache, w_gate, w_up)


def combine_call(attended, tokens, normed, early, ahead, w_gate, w_up, w_out, w_down):
    attended, normed, early, ahead = (pltpu.with_memory_space_constraint(a, pltpu.VMEM) for a in (attended, normed, early, ahead))
    batch, width = tokens.shape
    n_chunks = width // CHUNK_COLS
    dma = pltpu.SemaphoreType.DMA
    return pl.pallas_call(
        combine_kernel,
        name="combine",
        out_shape=pltpu.VMEM((batch, width), BF16),
        in_specs=[VM, ANY, VM, VM, VM, ANY, ANY, ANY, ANY],
        out_specs=VM,
        scratch_shapes=[
            pltpu.VMEM((batch, w_out.shape[0] + w_down.shape[0]), BF16),
            pltpu.VMEM((C_SLOTS, width, BLOCK), BF16),
            pltpu.VMEM((6, batch, 128), BF16),
            pltpu.VMEM((2, 16, width), BF16),
            pltpu.VMEM((n_chunks, batch, CHUNK_COLS), F32),
            pltpu.VMEM((n_chunks, 128, CHUNK_COLS), F32),
            pltpu.VMEM((n_chunks, 32, CHUNK_COLS), F32),
            pltpu.VMEM((n_chunks, 32, CHUNK_COLS), F32),
            pltpu.VMEM((n_chunks, 16, CHUNK_COLS), F32),
            pltpu.VMEM((n_chunks, 16, CHUNK_COLS), F32),
            dma((2,)), dma((C_SLOTS, 2)), dma((PEERS,)), dma((PEERS,)),
            dma((10, n_chunks)), dma((10, n_chunks)),
        ],
        compiler_params=pltpu.CompilerParams(collective_id=1, has_side_effects=True, vmem_limit_bytes=40 << 20),
    )(attended, tokens, normed, early, ahead, w_gate, w_up, w_out, w_down)


def solution(mesh):
    def local_step(tokens, lengths, k_cache, v_cache, norm_gain, w_query, w_key, w_value, w_out, w_gate, w_up, w_down):
        rows = tokens.shape[0] // PEERS
        q_all, key_new, value_new, normed, early = project_call(tokens, lengths, norm_gain, w_query, w_key, w_value, w_gate, w_up)
        attended, key_new, value_new, ahead = attend_call(lengths, q_all, key_new, value_new, k_cache, v_cache, w_gate, w_up)
        y = combine_call(attended, tokens, normed, early, ahead, w_gate, w_up, w_out, w_down)
        return y, key_new.reshape(rows, 1, 128), value_new.reshape(rows, 1, 128)

    in_specs = (P('replica', None), P('replica'), P('replica', None, None, None), P('replica', None, None, None), P(None), P(None, 'model'), P(None, None), P(None, None), P('model', None), P(None, 'model'), P(None, 'model'), P('model', None))
    out_specs = (P('replica', None), P(('replica', 'model'), None, None), P(('replica', 'model'), None, None))
    return jax.shard_map(local_step, mesh=mesh, in_specs=in_specs, out_specs=out_specs, check_vma=False)
```
